32 devices in a mesh: struct: 8 (over z, x), atom: 4 (over y, core).
Axes of the slice: x: 2, y: 2, z: 4, core: 2. Of those that a mesh axis runs over, the one named last changes fastest.
Arguments:
- atoms_in: bfloat16 [32, 1536, 128], P('struct', 'atom'), parts along dimension 0, may hold values from -6 to 6
- cond: bfloat16 [12288, 128], P(('struct', 'atom')), parts along dimension 0, may hold values from -6 to 6
- pair: bfloat16 [384, 32, 16, 128], P(('struct', 'atom')), parts along dimension 0, may hold values from -6 to 6
- atom_mask: int32 [12288], P(('struct', 'atom')), parts along dimension 0, may hold values 0 or 1
- atom_count: int32 [8], P('struct'), parts along dimension 0, may hold values from 1344 to 1536
- atom_to_token: int32 [12288], P(('struct', 'atom')), parts along dimension 0, may hold values from 0 to 191, as said below
- ada_weight: bfloat16 [2, 128, 256], replicated, may hold values from -0.5 to 0.5
- ada_bias: float32 [2, 128], replicated, may hold values from -1.5 to 1.5
- zero_weight: bfloat16 [2, 128, 128], replicated, may hold values from -0.5 to 0.5
- zero_bias: float32 [2, 128], replicated, may hold values from -2 to 2
- qkvg_weight: bfloat16 [128, 512], replicated, may hold values from -0.5 to 0.5
- query_bias: float32 [128], replicated, may hold values from -4 to 4
- pair_weight: float32 [4, 16], replicated, may hold values from -60 to 60
- out_weight: bfloat16 [128, 128], replicated, may hold values from -0.5 to 0.5
- swiglu_weight: bfloat16 [128, 512], replicated, may hold values from -0.5 to 0.5
- down_weight: bfloat16 [256, 128], replicated, may hold values from -0.375 to 0.375
- token_weight: bfloat16 [128, 768], replicated, may hold values from -0.5 to 0.5
Outputs:
- atoms_out: bfloat16 [32, 1536, 128], P('struct', 'atom'), parts along dimension 0
- tokens_out: bfloat16 [32, 192, 768], P('struct', 'atom'), parts along dimension 0
The draws below stay inside these ranges and needn't reach their ends.
There are 8 independent parts, one for each index of `struct`. The reference program is written for one: setup_inputs(seed, part) draws one part's arguments, and reference() takes and returns one part's arrays. A program takes and returns all parts, laid end to end along the dimension named above; an argument that names none is the same for every part. Nothing has to cross between parts.
Inputs may be any that keep to these rules, and one draw needn't show every extreme that they name: `atom_to_token`: never falls, rises by at most 1 from atom to atom, starts at 0 and ends at 191; an atom a of token t satisfies 8 * t - 8 < a < 8 * t + 2 * 8 - 1.
All inputs are finite; a program needn't handle non-finite values. No bound on the sum of `atom_mask` on one device may be relied on, other than what follows from the above.
Results may differ from the reference program's by a relative error of at most 0.01.
Values may be sent and summed in bfloat16 or wider, within the bound.
A program may use at most 64 MiB of HBM per device.

```python
import jax
import jax.numpy as jnp
from jax import lax

C = 128
HEADS = 4
CP = 16
FF = 256
CT = 768
WQ = 32
WK = 128
ATOMS_PER_TOKEN = 8
SAMPLES = 4
ATOM_DEV = 384
ATOMS = 1536
TOKENS = 192
WINDOWS = 48


def draw_atom_to_token(key, part):
    pairs = (TOKENS - 2) // 2
    size = jax.random.randint(jax.random.fold_in(key, 11), (pairs,), 1, ATOMS_PER_TOKEN)
    sign = 2 * jax.random.randint(jax.random.fold_in(key, 13), (pairs,), 0, 2) - 1
    jitter = size * sign
    middle = jnp.stack([ATOMS_PER_TOKEN + jitter, ATOMS_PER_TOKEN - jitter], axis=1).reshape(-1).astype(jnp.int32)
    edge_len = jnp.full((1,), ATOMS_PER_TOKEN, jnp.int32)
    lengths = jnp.concatenate([edge_len, middle, edge_len])
    return jnp.repeat(jnp.arange(TOKENS, dtype=jnp.int32), lengths, total_repeat_length=ATOMS)


def draw_pair_weight(key, part):
    values = jax.random.normal(jax.random.fold_in(key, 23), (HEADS, CP), jnp.float32)
    return jnp.clip(values * 0.5, -2.5, 2.5)


def place_ends(drawn, own_key, low, top_value):
    place = [jax.random.randint(jax.random.fold_in(own_key, axis), (), 0, length) for axis, length in enumerate(drawn.shape)]
    main_axis = drawn.shape.index(max(drawn.shape))
    beside = place[:main_axis] + [(place[main_axis] + 1) % drawn.shape[main_axis]] + place[main_axis + 1:]
    return drawn.at[tuple(place)].set(low).at[tuple(beside)].set(top_value)


def block_scale(rng, dims, split, least, top_value):
    loudness, own = 1.0, jax.random.fold_in(rng, 6)
    for axis_at, shards_of in split:
        heights = jnp.exp(jax.random.uniform(jax.random.fold_in(own, axis_at), (shards_of,), jnp.float32, least / len(split), top_value / len(split)))
        loudness = loudness * jnp.repeat(heights, dims[axis_at] // shards_of).reshape([-1 if axis == axis_at else 1 for axis in range(len(dims))])
    return loudness


def bell_draw(own_key, shape, scale, limit, shards=(), kind=jnp.bfloat16):
    entries = scale * jax.random.normal(own_key, shape, jnp.float32)
    if shards:
        entries = entries * block_scale(own_key, shape, shards, -0.22, 0.18)
    return jnp.clip(entries, -limit, limit).astype(kind)


def setup_inputs(seed: int = 0, part: int = 0) -> dict:
    key_list = jax.random.split(jax.random.key(seed), 18)
    own_keys = jax.random.split(jax.random.fold_in(key_list[17], part), 18)
    return {
        "atoms_in": bell_draw(own_keys[0], (SAMPLES, ATOMS, C), 1.0, 6.0, ((1, 4),)),
        "cond": bell_draw(own_keys[1], (ATOMS, C), 1.0, 6.0, ((0, 4),)),
        "pair": bell_draw(own_keys[2], (WINDOWS, WQ, CP, WK), 1.0, 6.0, ((0, 4),)),
        "atom_mask": place_ends((jax.random.randint(own_keys[3], (ATOMS,), 0, 16) < 15).astype(jnp.int32), jax.random.fold_in(own_keys[3], 1), 0, 1),
        "atom_count": jax.random.randint(own_keys[4], (1,), ATOMS - ATOM_DEV // 2, ATOMS + 1).astype(jnp.int32),
        "atom_to_token": draw_atom_to_token(jax.random.fold_in(jax.random.fold_in(key_list[17], part), 71), part),
        "ada_weight": bell_draw(key_list[6], (2, C, 2 * C), C ** -0.5, 0.5),
        "ada_bias": jnp.clip(jax.random.uniform(key_list[7], (2, C), jnp.float32, -1.5, 1.5), -1.5, 1.5),
        "zero_weight": bell_draw(key_list[8], (2, C, C), C ** -0.5, 0.5),
        "zero_bias": jnp.clip(jax.random.uniform(key_list[9], (2, C), jnp.float32, -2.0, 2.0), -2.0, 2.0),
        "qkvg_weight": bell_draw(key_list[10], (C, 4 * C), C ** -0.5, 0.5),
        "query_bias": bell_draw(key_list[11], (C,), 0.7, 4.0, (), jnp.float32),
        "pair_weight": draw_pair_weight(jax.random.fold_in(key_list[17], 71), part),
        "out_weight": bell_draw(key_list[13], (C, C), C ** -0.5, 0.5),
        "swiglu_weight": bell_draw(key_list[14], (C, 2 * FF), C ** -0.5, 0.5),
        "down_weight": bell_draw(key_list[15], (FF, C), FF ** -0.5, 0.375),
        "token_weight": bell_draw(key_list[16], (C, CT), C ** -0.5, 0.5),
    }


EPS = 1e-05

def layer_norm(values, along=-1):
    center = lax.optimization_barrier(jnp.mean(values, along, keepdims=True))
    spread = lax.optimization_barrier(jnp.mean(jnp.square(values - center), along, keepdims=True))
    return (values - center) * lax.rsqrt(spread + EPS)

def window_view(extended):
    reach = WK // WQ
    blocks = extended.reshape((WINDOWS + reach - 1, WQ) + extended.shape[1:])
    return jnp.concatenate([blocks[offset:offset + WINDOWS] for offset in range(reach)], axis=1)

def reference(atoms_in, cond, pair, atom_mask, atom_count, atom_to_token, ada_weight, ada_bias, zero_weight, zero_bias, qkvg_weight, query_bias, pair_weight, out_weight, swiglu_weight, down_weight, token_weight):
    head_dim = C // HEADS
    margin = (WK - WQ) // 2
    positions = jnp.arange(ATOMS, dtype=jnp.int32)
    usable = (atom_mask == 1) & (positions < atom_count[0])
    cond_norm = layer_norm(cond.astype(jnp.float32)).astype(jnp.bfloat16)
    adapt = [jnp.dot(cond_norm, ada_weight[which], preferred_element_type=jnp.float32) for which in range(2)]
    gating = [jax.nn.sigmoid(jnp.dot(cond_norm, zero_weight[which], preferred_element_type=jnp.float32) + zero_bias[which]) for which in range(2)]

    def adaptive(stream, which):
        return layer_norm(stream) * jax.nn.sigmoid(adapt[which][:, :C] + ada_bias[which]) + adapt[which][:, C:]
    key_live = window_view(jnp.pad(usable, (margin, margin)))
    pair_norm = layer_norm(pair.astype(jnp.float32), 2)
    pair_bias = jnp.einsum('wicj,hc->whij', pair_norm, pair_weight, precision=lax.Precision.HIGHEST)
    factor = head_dim ** (-0.5)

    def one_sample(stream):
        attn_in = adaptive(stream.astype(jnp.float32), 0).astype(jnp.bfloat16)
        projected = jnp.dot(attn_in, qkvg_weight, preferred_element_type=jnp.float32)
        queries = ((projected[:, :C] + query_bias) * factor).astype(jnp.bfloat16)
        keyval = projected[:, C:3 * C].astype(jnp.bfloat16)
        gate_attn = jax.nn.sigmoid(projected[:, 3 * C:])
        windowed = window_view(jnp.pad(keyval, ((margin, margin), (0, 0))))
        query_win = queries.reshape(WINDOWS, WQ, HEADS, head_dim).astype(jnp.float32)
        keys_win = windowed[..., :C].reshape(WINDOWS, WK, HEADS, head_dim).astype(jnp.float32)
        values_win = windowed[..., C:].reshape(WINDOWS, WK, HEADS, head_dim).astype(jnp.float32)
        scores = jnp.einsum('wihd,wjhd->whij', query_win, keys_win) + pair_bias
        scores = jnp.where(key_live[:, None, None, :], scores, -1000000000.0)
        attention = jax.nn.softmax(scores, axis=-1).astype(jnp.bfloat16)
        weighted = jnp.einsum('whij,wjhd->wihd', attention.astype(jnp.float32), values_win).reshape(ATOMS, C)
        blended = (weighted * gate_attn).astype(jnp.bfloat16)
        after_attn = (stream.astype(jnp.float32) + gating[0] * jnp.dot(blended, out_weight, preferred_element_type=jnp.float32)).astype(jnp.bfloat16)
        trans_in = adaptive(after_attn.astype(jnp.float32), 1).astype(jnp.bfloat16)
        mixed = jnp.dot(trans_in, swiglu_weight, preferred_element_type=jnp.float32)
        hidden = (jax.nn.silu(mixed[:, :FF]) * mixed[:, FF:]).astype(jnp.bfloat16)
        result = (after_attn.astype(jnp.float32) + gating[1] * jnp.dot(hidden, down_weight, preferred_element_type=jnp.float32)).astype(jnp.bfloat16)
        features = jax.nn.relu(jnp.dot(result, token_weight, preferred_element_type=jnp.float32)).astype(jnp.bfloat16)
        masked = jnp.where(usable[:, None], features.astype(jnp.float32), jnp.zeros((), jnp.float32))
        totals = jax.ops.segment_sum(masked, atom_to_token, num_segments=TOKENS)
        return (result, totals)
    atoms_out, totals = lax.map(one_sample, atoms_in)
    counts = jax.ops.segment_sum(usable.astype(jnp.float32), atom_to_token, num_segments=TOKENS)
    tokens_out = (totals / jnp.maximum(counts, 1.0)[None, :, None]).astype(jnp.bfloat16)
    return (atoms_out, tokens_out)
```

```python
import functools

import jax
import jax.numpy as jnp
from jax import lax
from jax.experimental import pallas as pl
from jax.experimental.pallas import tpu as pltpu
from jax.sharding import PartitionSpec as P

ATOMS_PER_TOKEN = 8
EPS = 1e-05
DEAD = -1e30
MIX_LAG = 2
BLEND_LAG = 1
MESH = pl.DeviceIdType.MESH
F32 = jnp.float32
BF16 = jnp.bfloat16


def iota(shape, axis):
    return lax.broadcasted_iota(jnp.int32, shape, axis)


def mm(a, b):
    return jnp.dot(a, b, preferred_element_type=F32)


def two_pieces(values):
    high = values.astype(BF16)
    low = (values - high.astype(F32)).astype(BF16)
    return high, low


def block_body(
    n,
    atoms_hbm, cond_hbm, pair_ref, mask_hbm, token_hbm, count_ref,
    ada_hbm, ada_bias_hbm, zero_hbm, zero_bias_hbm, qkvg_hbm, query_bias_hbm,
    pair_weight_hbm, out_hbm, swiglu_hbm, down_hbm, token_weight_hbm,
    atoms_out_ref, tokens_out_ref,
    atoms_ref, cond_ref, ada_ref, ada_bias_ref, zero_ref, zero_bias_ref, qkvg_ref,
    query_bias_ref, pair_weight_ref, out_ref, swiglu_ref, down_ref, token_weight_ref,
    mask_ref, token_ref,
    pair_buf, halo_x, halo_c, halo_m0, halo_m1, halo_t0, halo_t1, kv_ref, q_ref, gate_ref, bias_ref,
    mod_ref, feat_ref, blend_ref, center_ref, mean_ref, lhs_ref,
    edge_out, edge_in, onehot_ref, counts_ref,
    load_sem, pair_sem, send_sem, recv_sem, edge_send_sem, edge_recv_sem,
):
    samples, atoms, width = atoms_ref.shape
    windows, rows_pair, key_len = pair_ref.shape
    heads, channels = pair_weight_ref.shape
    head_dim = width // heads
    query_len = rows_pair // channels
    half = query_len // 2
    margin = (key_len - query_len) // 2
    tokens = tokens_out_ref.shape[1]
    hidden = down_ref.shape[0]
    token_width = token_weight_ref.shape[1]
    rows_half = half * channels

    halo_m, halo_t = (halo_m0, halo_m1), (halo_t0, halo_t1)
    me = lax.axis_index("atom")
    right, left = lax.rem(me + 1, n), lax.rem(me + n - 1, n)

    barrier = pltpu.get_barrier_semaphore()
    for neighbour in (left, right):
        pl.semaphore_signal(barrier, inc=1, device_id={"atom": neighbour}, device_id_type=MESH)

    early = (
        (cond_hbm, cond_ref), (atoms_hbm, atoms_ref), (ada_hbm, ada_ref),
        (ada_bias_hbm, ada_bias_ref), (zero_hbm, zero_ref), (zero_bias_hbm, zero_bias_ref),
        (qkvg_hbm, qkvg_ref), (query_bias_hbm, query_bias_ref),
        (pair_weight_hbm, pair_weight_ref), (mask_hbm, mask_ref), (token_hbm, token_ref),
    )
    late = (
        (out_hbm, out_ref), (swiglu_hbm, swiglu_ref), (down_hbm, down_ref),
        (token_weight_hbm, token_weight_ref),
    )
    loads = [
        pltpu.make_async_copy(src, dst, load_sem.at[i])
        for i, (src, dst) in enumerate(early + late)
    ]
    for copy in loads[: len(early)]:
        copy.start()
    groups = pair_sem.shape[0]
    per_group = windows // groups
    pair_copies = []
    for g in range(groups):
        part = pl.ds(g * per_group, per_group)
        copy = pltpu.make_async_copy(pair_ref.at[part], pair_buf.at[part], pair_sem.at[g])
        copy.start()
        pair_copies.append(copy)
    for copy in loads[len(early) :]:
        copy.start()

    row, col = iota((width, width), 0), iota((width, width), 1)
    inverse = 1.0 / width
    center_ref[...] = (jnp.where(row == col, 1.0, 0.0) - inverse).astype(BF16)
    mean_ref[...] = jnp.full(mean_ref.shape, inverse, F32).astype(BF16)
    kv_ref[:, :, 2 * width :] = jnp.ones((samples, atoms + 2 * margin, width), BF16)
    row, col = iota((rows_half, rows_half), 0), iota((rows_half, rows_half), 1)
    place = (row % half) * channels + row // half
    same = jnp.where(row % half == col // channels, 1.0 / channels, 0.0)
    lhs_ref[pl.ds(0, rows_half)] = (jnp.where(place == col, 1.0, 0.0) - same).astype(BF16)

    for copy in loads[: len(early)]:
        copy.wait()

    pl.semaphore_wait(barrier, 2)

    copies = []
    for side, (target, start) in enumerate(((right, atoms - margin), (left, 0))):
        own = pl.ds(start, margin)
        for which, (src, dst) in enumerate(
            (
                (atoms_ref.at[:, own], halo_x.at[side]),
                (cond_ref.at[own], halo_c.at[side]),
                (mask_ref, halo_m[side]),
                (token_ref, halo_t[side]),
            )
        ):
            copy = pltpu.make_async_remote_copy(
                src_ref=src,
                dst_ref=dst,
                send_sem=send_sem.at[side, which],
                recv_sem=recv_sem.at[side, which],
                device_id={"atom": target},
                device_id_type=MESH,
            )
            copy.start()
            copies.append(copy)

    def centre(values):
        return mm(values, center_ref[...])

    def scaled(centred):
        high, low = two_pieces(centred * centred)
        spread = mm(jnp.concatenate([high, low], axis=1), mean_ref[...])
        return centred * lax.rsqrt(spread + EPS)

    cond_centred = centre(cond_ref[...])
    atom_centred = [centre(atoms_ref[s]) for s in range(samples)]
    cond_norm = scaled(cond_centred).astype(BF16)
    normed = [scaled(c) for c in atom_centred]
    for which in range(2):
        adapt = mm(cond_norm, ada_ref[which])
        mod_ref[3 * which] = jax.nn.sigmoid(
            adapt[:, :width] + ada_bias_ref[which : which + 1]
        )
        mod_ref[3 * which + 1] = adapt[:, width:]
    zeroed = mm(cond_norm, jnp.concatenate([zero_ref[0], zero_ref[1]], axis=1))
    for which in range(2):
        mod_ref[3 * which + 2] = jax.nn.sigmoid(
            zeroed[:, which * width : (which + 1) * width] + zero_bias_ref[which : which + 1]
        )

    factor = head_dim**-0.5
    for s in range(samples):
        attn_in = (normed[s] * mod_ref[0] + mod_ref[1]).astype(BF16)
        projected = mm(attn_in, qkvg_ref[...])
        q_ref[s] = ((projected[:, :width] + query_bias_ref[...]) * factor).astype(BF16)
        kv_ref[s, pl.ds(margin, atoms), pl.ds(0, 2 * width)] = projected[
            :, width : 3 * width
        ].astype(BF16)
        gate_ref[s] = jax.nn.sigmoid(projected[:, 3 * width :])

    weight = pair_weight_ref[...]
    weight = weight - jnp.mean(weight, axis=1, keepdims=True)
    spread_c = jnp.where(
        iota((channels, rows_half), 1) % channels == iota((channels, rows_half), 0), 1.0, 0.0
    ).astype(BF16)
    own_query = iota((half, rows_half), 1) // channels == iota((half, rows_half), 0)
    remaining = weight
    lines = heads * half
    for piece in range(3):
        part = remaining.astype(BF16)
        remaining = remaining - part.astype(F32)
        wide = mm(part, spread_c)
        blocks = [
            jnp.where(own_query, jnp.broadcast_to(wide[h : h + 1], (half, rows_half)), 0.0)
            for h in range(heads)
        ]
        lhs_ref[pl.ds(rows_half + piece * lines, lines)] = jnp.concatenate(
            blocks, axis=0
        ).astype(BF16)

    def pair_window(w, live):
        block = pair_buf[w]
        both = jnp.concatenate([block[:rows_half], block[rows_half:]], axis=1)
        result = mm(lhs_ref[...], both)
        square = None
        for c in range(channels):
            centred = result[c * half : (c + 1) * half]
            square = centred * centred if c == 0 else square + centred * centred
        at = rows_half
        total = (
            result[at : at + lines]
            + result[at + lines : at + 2 * lines]
            + result[at + 2 * lines : at + 3 * lines]
        )
        scale = lax.rsqrt(square * (1.0 / channels) + EPS)
        bias = total * jnp.concatenate([scale] * heads, axis=0)
        keep = jnp.concatenate([live, live], axis=1)[0:1] > 0.5
        bias = jnp.where(keep, bias, DEAD)
        bias_ref[w, pl.ds(0, lines)] = bias[:, :key_len]
        bias_ref[w, pl.ds(lines, lines)] = bias[:, key_len:]

    def as_row(ref):
        return ref[...].reshape(1, atoms)

    def usable_at(mask, position):
        return (
            (mask == 1)
            & (position >= 0)
            & (position < n * atoms)
            & (position < count_ref[0])
        )

    inner = [
        w
        for w in range(windows)
        if w * query_len >= margin and w * query_len - margin + key_len <= atoms
    ]
    outer = [w for w in range(windows) if w not in inner]
    usable = usable_at(as_row(mask_ref), me * atoms + iota((1, atoms), 1))
    live = jnp.broadcast_to(jnp.where(usable, 1.0, 0.0), (8, atoms))
    for copy in pair_copies:
        copy.wait()
    for w in inner:
        start = w * query_len - margin
        pair_window(w, pltpu.roll(live, (atoms - start) % atoms, axis=1)[:, :key_len])

    for copy in loads[len(early) :]:
        copy.wait()
    for copy in copies:
        copy.wait()
    lanes = 128

    halo_centred = [
        centre(ref[...])
        for ref in (halo_c.at[0], halo_c.at[1])
    ] + [centre(halo_x[side].reshape(samples * margin, width)) for side in range(2)]

    mask_ext = jnp.concatenate(
        [as_row(halo_m[0])[:, atoms - lanes :], as_row(mask_ref), as_row(halo_m[1])[:, :lanes]],
        axis=1,
    )
    token_ext = jnp.concatenate(
        [as_row(halo_t[0])[:, atoms - lanes :], as_row(token_ref), as_row(halo_t[1])[:, :lanes]],
        axis=1,
    )
    extent = atoms + 2 * lanes
    usable = usable_at(mask_ext, me * atoms - lanes + iota((1, extent), 1))
    live = jnp.broadcast_to(jnp.where(usable, 1.0, 0.0), (8, extent))

    def outer_pair(w):
        shift = (extent - (lanes - margin + query_len * w)) % extent
        pair_window(w, pltpu.roll(live, shift, axis=1)[:, :key_len])

    pending = list(outer)
    if pending:
        outer_pair(pending.pop(0))
    halo_normed = [scaled(c) for c in halo_centred]
    if pending:
        outer_pair(pending.pop(0))
    halo_adapt = [mm(halo_normed[side].astype(BF16), ada_ref[0]) for side in range(2)]
    while pending:
        outer_pair(pending.pop(0))
    for side in range(2):
        inside = (me > 0) if side == 0 else (me < n - 1)
        scale = jax.nn.sigmoid(halo_adapt[side][:, :width] + ada_bias_ref[0:1])
        shift = halo_adapt[side][:, width:]
        attn_in = (
            halo_normed[2 + side].reshape(samples, margin, width) * scale[None] + shift[None]
        ).astype(BF16)
        projected = mm(
            attn_in.reshape(samples * margin, width), qkvg_ref[:, pl.ds(width, 2 * width)]
        )
        projected = jnp.where(inside, projected, 0.0).astype(BF16)
        start = 0 if side == 0 else margin + atoms
        kv_ref[:, pl.ds(start, margin), pl.ds(0, 2 * width)] = projected.reshape(
            samples, margin, 2 * width
        )

    relative = jnp.where(usable, token_ext - me * tokens, -2)
    hits = iota((tokens, extent), 0) == jnp.broadcast_to(relative, (tokens, extent))
    hits = jnp.where(hits, 1.0, 0.0)
    counts_ref[...] = jnp.broadcast_to(
        1.0 / jnp.maximum(jnp.sum(hits, axis=1, keepdims=True), 1.0), counts_ref.shape
    )
    onehot_ref[...] = hits[:, lanes : lanes + atoms].astype(BF16)
    relative8 = jnp.broadcast_to(relative[:, lanes : lanes + atoms], (8, atoms))
    rolled8 = pltpu.roll(relative8, query_len, axis=1)
    lower_hit = jnp.where(relative8[:, :lanes] == -1, 1.0, 0.0).astype(BF16)[:, :query_len]
    upper_hit = jnp.where(rolled8[:, :lanes] == tokens, 1.0, 0.0).astype(BF16)[:, :query_len]

    head_of = iota((half, width), 1) // head_dim
    blank = jnp.zeros((key_len, width), BF16)

    def stacked(s, w):
        query = q_ref[s, pl.ds(w * query_len, query_len)]
        parts = []
        for side in range(2):
            piece = query[side * half : (side + 1) * half]
            for h in range(heads):
                parts.append(jnp.where(head_of == h, piece, jnp.zeros_like(piece)))
        return jnp.concatenate(parts, axis=0)

    def score(w, group):
        keys = pl.ds(w * query_len, key_len)
        bias = bias_ref[w]
        both = jnp.concatenate([stacked(s, w) for s in group], axis=1)
        tall = jnp.concatenate(
            [
                jnp.concatenate(
                    [kv_ref[s, keys, pl.ds(0, width)] if t == s else blank for t in group], axis=1
                )
                for s in group
            ],
            axis=0,
        )
        scores = lax.dot_general(
            both, tall, (((1,), (1,)), ((), ())), preferred_element_type=F32
        )
        found = []
        for i in range(len(group)):
            own = scores[:, i * key_len : (i + 1) * key_len] + bias
            found.append((own, jnp.max(own, axis=1, keepdims=True)))
        return found

    def mix(w, group, found):
        keys = pl.ds(w * query_len, key_len)
        return [
            mm(jnp.exp(own - top).astype(BF16), kv_ref[s, keys, pl.ds(width, 2 * width)])
            for s, (own, top) in zip(group, found)
        ]

    def blend(w, group, mixes):
        rows = pl.ds(w * query_len, query_len)
        for s, mixed in zip(group, mixes):
            outs = []
            for side in range(2):
                base = side * heads * half
                value = mixed[base : base + half, :width]
                amount = mixed[base : base + half, width:]
                for h in range(1, heads):
                    at = base + h * half
                    value = jnp.where(head_of == h, mixed[at : at + half, :width], value)
                    amount = jnp.where(head_of == h, mixed[at : at + half, width:], amount)
                outs.append(value / amount)
            blend_ref[s, rows] = (jnp.concatenate(outs, axis=0) * gate_ref[s, rows]).astype(BF16)

    def transition(parts):
        def gather(ref):
            return jnp.concatenate([ref[s, pl.ds(a, m)] for s, a, m in parts], axis=0)

        def modulation(k):
            return jnp.concatenate([mod_ref[k, pl.ds(a, m)] for _, a, m in parts], axis=0)

        mixed = mm(gather(blend_ref), out_ref[...])
        yield
        after = (gather(atoms_ref).astype(F32) + modulation(2) * mixed).astype(BF16)
        centred = centre(after)
        yield
        trans_in = scaled(centred)
        yield
        trans_in = (trans_in * modulation(3) + modulation(4)).astype(BF16)
        mixed = mm(trans_in, swiglu_ref[...])
        yield
        units = (jax.nn.silu(mixed[:, :hidden]) * mixed[:, hidden:]).astype(BF16)
        mixed = mm(units, down_ref[...])
        yield
        final = (after.astype(F32) + modulation(5) * mixed).astype(BF16)
        features = jnp.maximum(mm(final, token_weight_ref[...]), 0.0).astype(BF16)
        at = 0
        for s, a, m in parts:
            atoms_out_ref[s, pl.ds(a, m)] = final[at : at + m]
            feat_ref[s, pl.ds(a, m)] = features[at : at + m]
            at += m
        yield

    edge_copies = []

    def edges():
        last = atoms - query_len
        parts = [(s, a, query_len) for s in range(samples) for a in (0, last)]
        yield from transition(parts)
        sample_row = iota((8, token_width), 0)
        for side, hit in enumerate((upper_hit, lower_hit)):
            total = jnp.zeros((8, token_width), F32)
            for s in range(samples):
                rows = pl.ds(last if side == 0 else 0, query_len)
                total = jnp.where(sample_row == s, mm(hit, feat_ref[s, rows]), total)
            edge_out[side] = total
        for side, target in enumerate((right, left)):
            copy = pltpu.make_async_remote_copy(
                src_ref=edge_out.at[side],
                dst_ref=edge_in.at[side],
                send_sem=edge_send_sem.at[side],
                recv_sem=edge_recv_sem.at[side],
                device_id={"atom": target},
                device_id_type=MESH,
            )
            copy.start()
            edge_copies.append(copy)
        yield

    ends = [0, windows - 1]
    order = ends + [w for w in range(windows) if w not in ends]
    units = [(w, (s, s + 1)) for w in order for s in range(0, samples, 2)]
    ready = len(ends) * samples // 2
    found, mixes = {}, {}
    edge_steps = edges()
    for i in range(len(units) + MIX_LAG + BLEND_LAG):
        if i < len(units):
            found[i] = score(*units[i])
        j = i - MIX_LAG
        if 0 <= j < len(units):
            mixes[j] = mix(*units[j], found.pop(j))
        j = j - BLEND_LAG
        if 0 <= j < len(units):
            blend(*units[j], mixes.pop(j))
        if j >= ready:
            next(edge_steps, None)
    for _ in edge_steps:
        pass

    middle = [(s, query_len, atoms - 2 * query_len) for s in range(samples)]
    for _ in transition(middle):
        pass

    for copy in edge_copies:
        copy.wait()
    token_row = iota((tokens, token_width), 0)
    per_count = counts_ref[:, 0:1]
    for s in range(samples):
        total = mm(onehot_ref[...], feat_ref[s])
        from_left = jnp.where(me > 0, edge_in[0, s : s + 1], 0.0)
        from_right = jnp.where(me < n - 1, edge_in[1, s : s + 1], 0.0)
        total = total + jnp.where(token_row == 0, from_left, 0.0)
        total = total + jnp.where(token_row == tokens - 1, from_right, 0.0)
        tokens_out_ref[s] = (total * per_count).astype(BF16)


def on_device(
    n,
    atoms_in, cond, pair, atom_mask, atom_count, atom_to_token, ada_weight, ada_bias,
    zero_weight, zero_bias, qkvg_weight, query_bias, pair_weight, out_weight,
    swiglu_weight, down_weight, token_weight,
):
    samples, atoms, width = atoms_in.shape
    windows, query_len, channels, key_len = pair.shape
    heads = pair_weight.shape[0]
    margin = (key_len - query_len) // 2
    tokens = atoms // ATOMS_PER_TOKEN
    token_width = token_weight.shape[1]
    half = query_len // 2
    rows_half = half * channels
    groups = 3 if windows % 6 == 0 else 1
    vmem = pl.BlockSpec(memory_space=pltpu.VMEM)
    hbm = pl.BlockSpec(memory_space=pltpu.HBM)
    query_bias = query_bias.reshape(1, width)
    staged = (
        atoms_in, cond, ada_weight, ada_bias, zero_weight, zero_bias, qkvg_weight,
        query_bias, pair_weight, out_weight, swiglu_weight, down_weight, token_weight,
        atom_mask, atom_to_token,
    )
    smem = pl.BlockSpec(memory_space=pltpu.SMEM)
    return pl.pallas_call(
        functools.partial(block_body, n),
        out_shape=(
            pltpu.VMEM(atoms_in.shape, BF16),
            pltpu.VMEM((samples, tokens, token_width), BF16),
        ),
        in_specs=[hbm, hbm, hbm, hbm, hbm, smem] + [hbm] * 11,
        out_specs=(vmem, vmem),
        scratch_shapes=[pltpu.VMEM(a.shape, a.dtype) for a in staged]
        + [
            pltpu.VMEM((windows, query_len * channels, key_len), BF16),
            pltpu.VMEM((2, samples, margin, width), BF16),
            pltpu.VMEM((2, margin, width), BF16),
            pltpu.VMEM((atoms,), jnp.int32),
            pltpu.VMEM((atoms,), jnp.int32),
            pltpu.VMEM((atoms,), jnp.int32),
            pltpu.VMEM((atoms,), jnp.int32),
            pltpu.VMEM((samples, atoms + 2 * margin, 3 * width), BF16),
            pltpu.VMEM((samples, atoms, width), BF16),
            pltpu.VMEM((samples, atoms, width), F32),
            pltpu.VMEM((windows, heads * query_len, key_len), F32),
            pltpu.VMEM((6, atoms, width), F32),
            pltpu.VMEM((samples, atoms, token_width), BF16),
            pltpu.VMEM((samples, atoms, width), BF16),
            pltpu.VMEM((width, width), BF16),
            pltpu.VMEM((2 * width, width), BF16),
            pltpu.VMEM((rows_half + 3 * heads * half, rows_half), BF16),
            pltpu.VMEM((2, 8, token_width), F32),
            pltpu.VMEM((2, 8, token_width), F32),
            pltpu.VMEM((tokens, atoms), BF16),
            pltpu.VMEM((tokens, 128), F32),
            pltpu.SemaphoreType.DMA((len(staged),)),
            pltpu.SemaphoreType.DMA((groups,)),
            pltpu.SemaphoreType.DMA((2, 4)),
            pltpu.SemaphoreType.DMA((2, 4)),
            pltpu.SemaphoreType.DMA((2,)),
            pltpu.SemaphoreType.DMA((2,)),
        ],
        compiler_params=pltpu.CompilerParams(collective_id=0, has_side_effects=True),
        name="atom_block",
    )(
        atoms_in, cond, pair.reshape(windows, query_len * channels, key_len),
        atom_mask, atom_to_token, atom_count,
        ada_weight, ada_bias, zero_weight, zero_bias, qkvg_weight,
        query_bias, pair_weight, out_weight, swiglu_weight,
        down_weight, token_weight,
    )


def solution(mesh):
    shard = P(("struct", "atom"))
    stream = P("struct", "atom", None)
    in_specs = (stream, shard, shard, shard, P("struct"), shard) + (P(),) * 11
    return jax.shard_map(
        functools.partial(on_device, mesh.shape["atom"]),
        mesh=mesh,
        in_specs=in_specs,
        out_specs=(stream, stream),
        check_vma=False,
    )
```

```python
import functools

import jax
import jax.numpy as jnp
from jax import lax
from jax.experimental import pallas as pl
from jax.experimental.pallas import tpu as pltpu
from jax.sharding import PartitionSpec as P

ATOMS_PER_TOKEN = 8
EPS = 1e-05
DEAD = -1e30
MIX_LAG = 2
BLEND_LAG = 1
FILL_HALO = 2
FILL_EVERY = 2
MESH = pl.DeviceIdType.MESH
F32 = jnp.float32
BF16 = jnp.bfloat16


def iota(shape, axis):
    return lax.broadcasted_iota(jnp.int32, shape, axis)


def mm(a, b):
    return jnp.dot(a, b, preferred_element_type=F32)


def block_body(
    n,
    atoms_hbm, cond_hbm, pair_ref, mask_hbm, token_hbm, count_hbm,
    ada_hbm, ada_bias_hbm, zero_hbm, zero_bias_hbm, qkvg_hbm, query_bias_hbm,
    pair_weight_hbm, out_hbm, swiglu_hbm, down_hbm, token_weight_hbm,
    atoms_out_ref, tokens_out_ref,
    cond_ref, ada_ref, ada_bias_ref, zero_ref, zero_bias_ref, qkvg_ref,
    query_bias_ref, pair_weight_ref, out_ref, swiglu_ref, down_ref, token_weight_ref,
    mask_ref, token_ref, count_ref, atoms_ref,
    pair_buf, pair_far, halo_x, halo_c, halo_m0, halo_m1, halo_t0, halo_t1,
    kv_ref, q_ref, gate_ref, bias_ref, mod_ref, feat_ref, blend_ref, lhs_ref,
    load_sem, pair_sem, send_sem, recv_sem,
):
    samples, atoms, width = atoms_out_ref.shape
    windows, rows_pair, key_len = pair_ref.shape
    heads, channels = pair_weight_ref.shape
    head_dim = width // heads
    query_len = rows_pair // channels
    half = query_len // 2
    margin = (key_len - query_len) // 2
    wide = margin + query_len
    reach = ATOMS_PER_TOKEN
    tokens = tokens_out_ref.shape[1]
    hidden = down_ref.shape[0]
    rows_half = half * channels
    lines = heads * half
    lanes = 128

    halo_m, halo_t = (halo_m0, halo_m1), (halo_t0, halo_t1)
    me = lax.axis_index("atom")
    right, left = lax.rem(me + 1, n), lax.rem(me + n - 1, n)

    barrier = pltpu.get_barrier_semaphore()
    has_left, has_right = me > 0, me < n - 1

    @pl.when(has_left)
    def _():
        pl.semaphore_signal(barrier, inc=1, device_id={"atom": left}, device_id_type=MESH)

    @pl.when(has_right)
    def _():
        pl.semaphore_signal(barrier, inc=1, device_id={"atom": right}, device_id_type=MESH)


    early = (
        (cond_hbm, cond_ref), (atoms_hbm, atoms_ref.at[:, pl.ds(0, atoms)]), (ada_hbm, ada_ref),
        (ada_bias_hbm, ada_bias_ref), (zero_hbm, zero_ref), (zero_bias_hbm, zero_bias_ref),
        (qkvg_hbm, qkvg_ref), (query_bias_hbm, query_bias_ref),
        (pair_weight_hbm, pair_weight_ref), (mask_hbm, mask_ref), (token_hbm, token_ref),
        (count_hbm, count_ref),
    )
    late = (
        (out_hbm, out_ref), (swiglu_hbm, swiglu_ref), (down_hbm, down_ref),
        (token_weight_hbm, token_weight_ref),
    )
    loads = [
        pltpu.make_async_copy(src, dst, load_sem.at[i])
        for i, (src, dst) in enumerate(early + late)
    ]
    for copy in loads[: len(early)]:
        copy.start()
    pair_copies = [pltpu.make_async_copy(pair_ref, pair_buf, pair_sem.at[0])]
    pair_copies[0].start()
    for copy in loads[len(early) :]:
        copy.start()

    inverse = 1.0 / width
    kv_ref[:, :, 2 * width :] = jnp.ones((samples, atoms + 2 * wide, width), BF16)
    row, col = iota((rows_half, rows_half), 0), iota((rows_half, rows_half), 1)
    place = (row % half) * channels + row // half
    same = jnp.where(row % half == col // channels, 1.0 / channels, 0.0)
    lhs_ref[pl.ds(0, rows_half)] = (jnp.where(place == col, 1.0, 0.0) - same).astype(BF16)

    skipped = rows_half - reach * channels
    pair_far[pl.ds(0, skipped)] = jnp.zeros((skipped, key_len), BF16)
    pair_far[pl.ds(2 * rows_half - skipped, skipped)] = jnp.zeros((skipped, key_len), BF16)
    for side, there in enumerate((has_left, has_right)):

        @pl.when(jnp.logical_not(there))
        def _(side=side):
            at = skipped + side * reach * channels
            pair_far[pl.ds(at, reach * channels)] = jnp.zeros((reach * channels, key_len), BF16)
            halo_x[side] = jnp.zeros(halo_x.shape[1:], BF16)
            halo_c[side] = jnp.zeros(halo_c.shape[1:], BF16)
            halo_m[side][...] = jnp.zeros(halo_m0.shape, jnp.int32)
            halo_t[side][...] = jnp.zeros(halo_t0.shape, jnp.int32)

    copies = []
    for side, (target, start, far) in enumerate(
        ((right, atoms - wide, (windows - 1, rows_pair - reach * channels)), (left, 0, (0, 0)))
    ):
        own = pl.ds(start, wide)
        size = reach * channels
        for which, (src, dst) in enumerate(
            (
                (atoms_ref.at[:, own], halo_x.at[side]),
                (cond_ref.at[own], halo_c.at[side]),
                (mask_ref, halo_m[side]),
                (token_ref, halo_t[side]),
                (
                    pair_buf.at[far[0], pl.ds(far[1], size)],
                    pair_far.at[pl.ds(skipped + side * size, size)],
                ),
            )
        ):
            copies.append(
                pltpu.make_async_remote_copy(
                    src_ref=src,
                    dst_ref=dst,
                    send_sem=send_sem.at[side, which],
                    recv_sem=recv_sem.at[side, which],
                    device_id={"atom": target},
                    device_id_type=MESH,
                )
            )
    to_right, to_left = copies[:5], copies[5:]

    def sends(chosen):
        @pl.when(has_right)
        def _():
            for k in chosen:
                to_right[k].start()

        @pl.when(has_left)
        def _():
            for k in chosen:
                to_left[k].start()

    for copy in loads[: len(early)]:
        copy.wait()

    pl.semaphore_wait(barrier, (me + n - 1) // n + (2 * n - 2 - me) // n)

    sends(range(4))

    def norm(values):
        values = values.astype(F32)
        centred = values - jnp.sum(values, axis=1, keepdims=True) * inverse
        spread = jnp.sum(centred * centred, axis=1, keepdims=True) * inverse
        return centred * lax.rsqrt(spread + EPS)

    cond_norm = norm(cond_ref[...]).astype(BF16)
    normed = [norm(atoms_ref[s, pl.ds(0, atoms)]) for s in range(samples)]
    for which in range(2):
        adapt = mm(cond_norm, ada_ref[which])
        mod_ref[3 * which, pl.ds(0, atoms)] = jax.nn.sigmoid(
            adapt[:, :width] + ada_bias_ref[which : which + 1]
        )
        mod_ref[3 * which + 1, pl.ds(0, atoms)] = adapt[:, width:]
    zeroed = mm(cond_norm, jnp.concatenate([zero_ref[0], zero_ref[1]], axis=1))
    for which in range(2):
        mod_ref[3 * which + 2, pl.ds(0, atoms)] = jax.nn.sigmoid(
            zeroed[:, which * width : (which + 1) * width] + zero_bias_ref[which : which + 1]
        )

    factor = head_dim**-0.5

    def as_query(projected):
        return ((projected + query_bias_ref[...]) * factor).astype(BF16)

    own = pl.ds(0, atoms)
    for s in range(samples):
        attn_in = (normed[s] * mod_ref[0, own] + mod_ref[1, own]).astype(BF16)
        projected = mm(attn_in, qkvg_ref[...])
        q_ref[s, own] = as_query(projected[:, :width])
        kv_ref[s, pl.ds(wide, atoms), pl.ds(0, 2 * width)] = projected[
            :, width : 3 * width
        ].astype(BF16)
        gate_ref[s, own] = jax.nn.sigmoid(projected[:, 3 * width :])

    weight = pair_weight_ref[...]
    weight = weight - jnp.mean(weight, axis=1, keepdims=True)
    spread_c = jnp.where(
        iota((channels, rows_half), 1) % channels == iota((channels, rows_half), 0), 1.0, 0.0
    ).astype(BF16)
    own_query = iota((half, rows_half), 1) // channels == iota((half, rows_half), 0)
    remaining = weight
    for piece in range(3):
        part = remaining.astype(BF16)
        remaining = remaining - part.astype(F32)
        broad = mm(part, spread_c)
        blocks = [
            jnp.where(own_query, jnp.broadcast_to(broad[h : h + 1], (half, rows_half)), 0.0)
            for h in range(heads)
        ]
        lhs_ref[pl.ds(rows_half + piece * lines, lines)] = jnp.concatenate(
            blocks, axis=0
        ).astype(BF16)

    def pair_window(w, block, keep):
        both = jnp.concatenate([block[:rows_half], block[rows_half:]], axis=1)
        result = mm(lhs_ref[...], both)
        square = None
        for c in range(channels):
            centred = result[c * half : (c + 1) * half]
            square = centred * centred if c == 0 else square + centred * centred
        at = rows_half
        total = (
            result[at : at + lines]
            + result[at + lines : at + 2 * lines]
            + result[at + 2 * lines : at + 3 * lines]
        )
        scale = lax.rsqrt(square * (1.0 / channels) + EPS)
        bias = total * jnp.concatenate([scale] * heads, axis=0)
        if keep is not None:
            bias = jnp.where(jnp.concatenate(keep, axis=1)[0:1] > 0.5, bias, DEAD)
        bias_ref[w, pl.ds(0, lines)] = bias[:, :key_len]
        bias_ref[w, pl.ds(lines, lines)] = bias[:, key_len:]

    def as_row(ref):
        return ref[...].reshape(1, atoms)

    def usable_at(mask, position):
        return (
            (mask == 1)
            & (position >= 0)
            & (position < n * atoms)
            & (position < count_ref[0])
        )

    def alive(usable):
        return jnp.broadcast_to(jnp.where(usable, 1.0, 0.0), (8, usable.shape[1]))

    def lanes_from(row, start, size):
        length = row.shape[1]
        return pltpu.roll(row, (length - start) % length, axis=1)[:, :size]

    inner = [
        w
        for w in range(windows)
        if w * query_len >= margin and w * query_len - margin + key_len <= atoms
    ]
    outer = [w for w in range(windows) if w not in inner]
    live = alive(usable_at(as_row(mask_ref), me * atoms + iota((1, atoms), 1)))
    for copy in pair_copies:
        copy.wait()
    for copy in loads[len(early) :]:
        copy.wait()
    sends([4])
    for w in inner:
        pair_window(w, pair_buf[w], [lanes_from(live, w * query_len - margin, key_len)] * 2)
    for w in outer:
        pair_window(w, pair_buf[w], None)

    head_of = iota((half, width), 1) // head_dim
    blank = jnp.zeros((key_len, width), BF16)

    def tiles_of(w, s):
        return [(t, (w + 1) * query_len, w * query_len, query_len, w, 0) for t in (s, s + 1)]

    def far_tiles(s):
        return [
            (s, 0, atoms, half, windows, 0),
            (s, atoms + 2 * wide - key_len, atoms + half, half, windows, lines),
        ]

    def stacked(s, row, count):
        query = q_ref[s, pl.ds(row, count)]
        parts = []
        for at in range(0, count, half):
            piece = query[at : at + half]
            for h in range(heads):
                parts.append(jnp.where(head_of == h, piece, jnp.zeros_like(piece)))
        return jnp.concatenate(parts, axis=0)

    def score(tiles):
        both = jnp.concatenate([stacked(s, row, m) for s, _, row, m, _, _ in tiles], axis=1)
        tall = []
        for s, key, _, _, _, _ in tiles:
            line = [blank] * len(tiles)
            line[len(tall)] = kv_ref[s, pl.ds(key, key_len), pl.ds(0, width)]
            tall.append(jnp.concatenate(line, axis=1))
        scores = lax.dot_general(
            both,
            jnp.concatenate(tall, axis=0),
            (((1,), (1,)), ((), ())),
            preferred_element_type=F32,
        )
        found = []
        for i, (_, _, _, m, w, line) in enumerate(tiles):
            own = scores[:, i * key_len : (i + 1) * key_len]
            own = own + bias_ref[w, pl.ds(line, heads * m)]
            found.append((own, jnp.max(own, axis=1, keepdims=True)))
        return found

    def mix(tiles, found):
        return [
            mm(
                jnp.exp(own - top).astype(BF16),
                kv_ref[s, pl.ds(key, key_len), pl.ds(width, 2 * width)],
            )
            for (s, key, _, _, _, _), (own, top) in zip(tiles, found)
        ]

    def blend(tiles, mixes):
        for (s, _, row, m, _, _), mixed in zip(tiles, mixes):
            rows = pl.ds(row, m)
            outs = []
            for base in range(0, heads * m, lines):
                value = mixed[base : base + half, :width]
                amount = mixed[base : base + half, width:]
                for h in range(1, heads):
                    at = base + h * half
                    value = jnp.where(head_of == h, mixed[at : at + half, :width], value)
                    amount = jnp.where(head_of == h, mixed[at : at + half, width:], amount)
                outs.append(value / amount)
            blend_ref[s, rows] = (jnp.concatenate(outs, axis=0) * gate_ref[s, rows]).astype(BF16)

    def transition(parts):
        def gather(ref):
            return jnp.concatenate([ref[s, pl.ds(a, m)] for s, a, m in parts], axis=0)

        def modulation(k):
            return jnp.concatenate([mod_ref[k, pl.ds(a, m)] for _, a, m in parts], axis=0)

        mixed = mm(gather(blend_ref), out_ref[...])
        yield
        after = (gather(atoms_ref).astype(F32) + modulation(2) * mixed).astype(BF16)
        trans_in = (norm(after) * modulation(3) + modulation(4)).astype(BF16)
        mixed = mm(trans_in, swiglu_ref[...])
        yield
        units = (jax.nn.silu(mixed[:, :hidden]) * mixed[:, hidden:]).astype(BF16)
        mixed = mm(units, down_ref[...])
        yield
        final = (after.astype(F32) + modulation(5) * mixed).astype(BF16)
        features = jnp.maximum(mm(final, token_weight_ref[...]), 0.0).astype(BF16)
        at = 0
        for s, a, m in parts:
            kept = min(a + m, atoms) - a
            atoms_out_ref[s, pl.ds(a, kept)] = final[at : at + kept]
            feat_ref[s, pl.ds(a, m)] = features[at : at + m]
            at += m
        yield

    def attention(units):
        found, mixes = {}, {}
        for i in range(len(units) + MIX_LAG + BLEND_LAG):
            if i < len(units):
                found[i] = score(units[i])
            j = i - MIX_LAG
            if 0 <= j < len(units):
                mixes[j] = mix(units[j], found.pop(j))
            j = j - BLEND_LAG
            if 0 <= j < len(units):
                blend(units[j], mixes.pop(j))
            yield

    def rotate(streams):
        streams = list(streams)
        while streams:
            for stream in list(streams):
                if next(stream, streams) is streams:
                    streams.remove(stream)
                else:
                    yield

    for _ in attention([tiles_of(w, s) for w in inner for s in range(0, samples, 2)]):
        pass

    for to_there, out_there, in_there in (
        (to_right, has_right, has_left),
        (to_left, has_left, has_right),
    ):

        @pl.when(out_there)
        def _(copies=to_there):
            for copy in copies:
                copy.wait_send()

        @pl.when(in_there)
        def _(copies=to_there):
            for copy in copies:
                copy.wait_recv()

    extent = atoms + 2 * lanes

    def extended(halo, ref):
        return jnp.concatenate(
            [as_row(halo[0])[:, atoms - lanes :], as_row(ref), as_row(halo[1])[:, :lanes]],
            axis=1,
        )

    usable = usable_at(extended(halo_m, mask_ref), me * atoms - lanes + iota((1, extent), 1))
    relative = jnp.where(usable, extended(halo_t, token_ref) - me * tokens, -2)
    live = alive(usable)

    def halo():
        near = [pl.ds(wide - half, half), pl.ds(0, half)]
        for side in range(2):
            atoms_ref[:, pl.ds(atoms + side * half, half)] = halo_x[side, :, near[side]]
        cond_norm = norm(jnp.concatenate([halo_c[0], halo_c[1]], axis=0)).astype(BF16)
        normed = norm(
            jnp.concatenate(
                [halo_x[side].reshape(samples * wide, width) for side in range(2)], axis=0
            )
        ).reshape(2, samples, wide, width)
        adapt = mm(cond_norm, ada_ref[0])
        close = jnp.concatenate([cond_norm[wide - half : wide], cond_norm[wide : wide + half]], axis=0)
        close_adapt = mm(close, ada_ref[1])
        zeroed = mm(close, jnp.concatenate([zero_ref[0], zero_ref[1]], axis=1))
        far = [
            lanes_from(live, lanes - wide, key_len),
            lanes_from(live, lanes + atoms + wide - key_len, key_len),
        ]
        pair_window(windows, pair_far[...], far)
        yield
        for w in outer:
            keep = lanes_from(live, lanes + w * query_len - margin, key_len)[0:1] > 0.5
            bias_ref[w] = jnp.where(keep, bias_ref[w], DEAD)
        extra = pl.ds(atoms, 2 * half)
        mod_ref[3, extra] = jax.nn.sigmoid(close_adapt[:, :width] + ada_bias_ref[1:2])
        mod_ref[4, extra] = close_adapt[:, width:]
        for which in range(2):
            mod_ref[3 * which + 2, extra] = jax.nn.sigmoid(
                zeroed[:, which * width : (which + 1) * width] + zero_bias_ref[which : which + 1]
            )
        scale = jax.nn.sigmoid(adapt[:, :width] + ada_bias_ref[0:1])
        attn_in = (
            normed * scale.reshape(2, 1, wide, width)
            + adapt[:, width:].reshape(2, 1, wide, width)
        ).astype(BF16)
        projected = mm(
            attn_in.reshape(2 * samples * wide, width), qkvg_ref[:, pl.ds(width, 2 * width)]
        )
        close = jnp.concatenate(
            [
                attn_in[side, s, at : at + half]
                for s in range(samples)
                for side, at in enumerate((wide - half, 0))
            ],
            axis=0,
        )
        sides = mm(
            close,
            jnp.concatenate(
                [qkvg_ref[:, pl.ds(0, width)], qkvg_ref[:, pl.ds(3 * width, width)]], axis=1
            ),
        ).reshape(samples, 2 * half, 2 * width)
        yield
        for side, there in enumerate((has_left, has_right)):
            own = projected[side * samples * wide : (side + 1) * samples * wide]
            own = jnp.where(there, own, 0.0).astype(BF16)
            start = side * (wide + atoms)
            kv_ref[:, pl.ds(start, wide), pl.ds(0, 2 * width)] = own.reshape(
                samples, wide, 2 * width
            )
        for s in range(samples):
            q_ref[s, extra] = as_query(sides[s, :, :width])
            gate_ref[s, extra] = jax.nn.sigmoid(sides[s, :, width:])
        yield

    first, count = inner[0] * query_len, len(inner) * query_len
    fill = rotate([transition([(s, first, count)]) for s in range(samples)])
    for _ in halo():
        for _ in range(FILL_HALO):
            next(fill, None)
    units = [tiles_of(w, s) for w in outer for s in range(0, samples, 2)]
    units += [far_tiles(s) for s in range(samples)]
    for i, _ in enumerate(attention(units)):
        if i % FILL_EVERY == 0:
            next(fill, None)

    strip = iota((1, extent), 1)
    beyond = jnp.where(
        strip < half,
        pltpu.roll(jnp.broadcast_to(relative, (8, extent)), extent - lanes + half, axis=1)[0:1],
        pltpu.roll(jnp.broadcast_to(relative, (8, extent)), extent - lanes - atoms + half, axis=1)[0:1],
    )[:, : 2 * half]
    chosen = jnp.concatenate([relative[:, lanes : lanes + atoms], beyond], axis=1)
    total_atoms = atoms + 2 * half
    hits = iota((tokens, extent), 0) == jnp.broadcast_to(relative, (tokens, extent))
    per_count = 1.0 / jnp.maximum(
        jnp.sum(jnp.where(hits, 1.0, 0.0), axis=1, keepdims=True), 1.0
    )
    onehot = jnp.where(
        iota((tokens, total_atoms), 0) == jnp.broadcast_to(chosen, (tokens, total_atoms)), 1.0, 0.0
    ).astype(BF16)

    def closing(s):
        yield from transition(
            [(s, 0, first), (s, first + count, atoms - first - count + 2 * half)]
        )
        tokens_out_ref[s] = (mm(onehot, feat_ref[s]) * per_count).astype(BF16)
        yield

    for _ in rotate([fill] + [closing(s) for s in range(samples)]):
        pass


def on_device(
    n,
    atoms_in, cond, pair, atom_mask, atom_count, atom_to_token, ada_weight, ada_bias,
    zero_weight, zero_bias, qkvg_weight, query_bias, pair_weight, out_weight,
    swiglu_weight, down_weight, token_weight,
):
    samples, atoms, width = atoms_in.shape
    windows, query_len, channels, key_len = pair.shape
    heads = pair_weight.shape[0]
    wide = (key_len + query_len) // 2
    spread = atoms + query_len
    tokens = atoms // ATOMS_PER_TOKEN
    token_width = token_weight.shape[1]
    half = query_len // 2
    rows_half = half * channels
    vmem = pl.BlockSpec(memory_space=pltpu.VMEM)
    hbm = pl.BlockSpec(memory_space=pltpu.HBM)
    query_bias = query_bias.reshape(1, width)
    staged = (
        cond, ada_weight, ada_bias, zero_weight, zero_bias, qkvg_weight,
        query_bias, pair_weight, out_weight, swiglu_weight, down_weight, token_weight,
        atom_mask, atom_to_token,
    )
    return pl.pallas_call(
        functools.partial(block_body, n),
        out_shape=(
            pltpu.VMEM(atoms_in.shape, BF16),
            pltpu.VMEM((samples, tokens, token_width), BF16),
        ),
        in_specs=[hbm] * 17,
        out_specs=(vmem, vmem),
        scratch_shapes=[pltpu.VMEM(a.shape, a.dtype) for a in staged]
        + [
            pltpu.SMEM(atom_count.shape, atom_count.dtype),
            pltpu.VMEM((samples, spread, width), BF16),
            pltpu.VMEM((windows, query_len * channels, key_len), BF16),
            pltpu.VMEM((query_len * channels, key_len), BF16),
            pltpu.VMEM((2, samples, wide, width), BF16),
            pltpu.VMEM((2, wide, width), BF16),
            pltpu.VMEM((atoms,), jnp.int32),
            pltpu.VMEM((atoms,), jnp.int32),
            pltpu.VMEM((atoms,), jnp.int32),
            pltpu.VMEM((atoms,), jnp.int32),
            pltpu.VMEM((samples, atoms + 2 * wide, 3 * width), BF16),
            pltpu.VMEM((samples, spread, width), BF16),
            pltpu.VMEM((samples, spread, width), F32),
            pltpu.VMEM((windows + 1, heads * query_len, key_len), F32),
            pltpu.VMEM((6, spread, width), F32),
            pltpu.VMEM((samples, spread, token_width), BF16),
            pltpu.VMEM((samples, spread, width), BF16),
            pltpu.VMEM((rows_half + 3 * heads * half, rows_half), BF16),
            pltpu.SemaphoreType.DMA((len(staged) + 2,)),
            pltpu.SemaphoreType.DMA((1,)),
            pltpu.SemaphoreType.DMA((2, 5)),
            pltpu.SemaphoreType.DMA((2, 5)),
        ],
        compiler_params=pltpu.CompilerParams(collective_id=0, has_side_effects=True),
        name="atom_block",
    )(
        atoms_in, cond, pair.reshape(windows, query_len * channels, key_len),
        atom_mask, atom_to_token, atom_count,
        ada_weight, ada_bias, zero_weight, zero_bias, qkvg_weight,
        query_bias, pair_weight, out_weight, swiglu_weight,
        down_weight, token_weight,
    )


def solution(mesh):
    shard = P(("struct", "atom"))
    stream = P("struct", "atom", None)
    in_specs = (stream, shard, shard, shard, P("struct"), shard) + (P(),) * 11
    return jax.shard_map(
        functools.partial(on_device, mesh.shape["atom"]),
        mesh=mesh,
        in_specs=in_specs,
        out_specs=(stream, stream),
        check_vma=False,
    )
```

```python
import functools

import jax
import jax.numpy as jnp
from jax import lax
from jax.experimental import pallas as pl
from jax.experimental.pallas import tpu as pltpu
from jax.sharding import PartitionSpec as P

ATOMS_PER_TOKEN = 8
EPS = 1e-05
DEAD = -1e30
MIX_LAG = 4
BLEND_LAG = 1
AHEAD = 8
FILL_HALO = 2
FILL_EVERY = 2
MESH = pl.DeviceIdType.MESH
F32 = jnp.float32
BF16 = jnp.bfloat16


def iota(shape, axis):
    return lax.broadcasted_iota(jnp.int32, shape, axis)


def mm(a, b):
    return jnp.dot(a, b, preferred_element_type=F32)


def block_body(
    n,
    atoms_hbm, cond_hbm, pair_ref, mask_hbm, token_hbm, count_hbm,
    ada_hbm, ada_bias_hbm, zero_hbm, zero_bias_hbm, qkvg_hbm, query_bias_hbm,
    pair_weight_hbm, out_hbm, swiglu_hbm, down_hbm, token_weight_hbm,
    atoms_out_ref, tokens_out_ref,
    cond_ref, ada_ref, ada_bias_ref, zero_ref, zero_bias_ref, qkvg_ref,
    query_bias_ref, pair_weight_ref, out_ref, swiglu_ref, down_ref, token_weight_ref,
    mask_ref, token_ref, count_ref, atoms_ref,
    pair_buf, pair_far, halo_x, halo_c, halo_m0, halo_m1, halo_t0, halo_t1,
    kv_ref, q_ref, gate_ref, bias_ref, mod_ref, feat_ref, blend_ref, lhs_ref,
    load_sem, pair_sem, send_sem, recv_sem, ready_sem,
):
    samples, atoms, width = atoms_out_ref.shape
    windows, rows_pair, key_len = pair_ref.shape
    heads, channels = pair_weight_ref.shape
    head_dim = width // heads
    query_len = rows_pair // channels
    half = query_len // 2
    margin = (key_len - query_len) // 2
    wide = margin + query_len
    reach = ATOMS_PER_TOKEN
    tokens = tokens_out_ref.shape[1]
    hidden = down_ref.shape[0]
    rows_half = half * channels
    lines = heads * half
    lanes = 128

    halo_m, halo_t = (halo_m0, halo_m1), (halo_t0, halo_t1)
    me = lax.axis_index("atom")
    right, left = lax.rem(me + 1, n), lax.rem(me + n - 1, n)

    barrier = pltpu.get_barrier_semaphore()
    has_left, has_right = me > 0, me < n - 1

    @pl.when(has_right)
    def _():
        pl.semaphore_signal(barrier, inc=1, device_id={"atom": right}, device_id_type=MESH)


    pair_copy = pltpu.make_async_copy(pair_ref, pair_buf, pair_sem.at[0])
    early = (
        (cond_hbm, cond_ref), (atoms_hbm, atoms_ref.at[:, pl.ds(0, atoms)]), (ada_hbm, ada_ref),
        (ada_bias_hbm, ada_bias_ref), (zero_hbm, zero_ref), (zero_bias_hbm, zero_bias_ref),
        (qkvg_hbm, qkvg_ref), (query_bias_hbm, query_bias_ref), (mask_hbm, mask_ref),
        (token_hbm, token_ref), (pair_weight_hbm, pair_weight_ref), (count_hbm, count_ref),
    )
    late = (
        (out_hbm, out_ref), (swiglu_hbm, swiglu_ref), (down_hbm, down_ref),
        (token_weight_hbm, token_weight_ref),
    )
    loads = [
        pltpu.make_async_copy(src, dst, load_sem.at[i])
        for i, (src, dst) in enumerate(early + late)
    ]
    for copy in loads[: len(early)]:
        copy.start()
    pair_copy.start()
    for copy in loads[len(early) :]:
        copy.start()

    inverse = 1.0 / width
    kv_ref[:, :, 2 * width :] = jnp.ones((samples, atoms + 2 * wide, width), BF16)
    row, col = iota((rows_half, rows_half), 0), iota((rows_half, rows_half), 1)
    place = (row % half) * channels + row // half
    same = jnp.where(row % half == col // channels, 1.0 / channels, 0.0)
    lhs_ref[pl.ds(0, rows_half)] = (jnp.where(place == col, 1.0, 0.0) - same).astype(BF16)

    skipped = rows_half - reach * channels
    pair_far[pl.ds(0, skipped)] = jnp.zeros((skipped, key_len), BF16)
    pair_far[pl.ds(2 * rows_half - skipped, skipped)] = jnp.zeros((skipped, key_len), BF16)
    for side, there in enumerate((has_left, has_right)):

        @pl.when(jnp.logical_not(there))
        def _(side=side):
            at = skipped + side * reach * channels
            pair_far[pl.ds(at, reach * channels)] = jnp.zeros((reach * channels, key_len), BF16)
            halo_x[side] = jnp.zeros(halo_x.shape[1:], BF16)
            halo_c[side] = jnp.zeros(halo_c.shape[1:], BF16)
            halo_m[side][...] = jnp.zeros(halo_m0.shape, jnp.int32)
            halo_t[side][...] = jnp.zeros(halo_t0.shape, jnp.int32)

    copies = []
    for side, (target, start, far) in enumerate(
        ((right, atoms - wide, (windows - 1, rows_pair - reach * channels)), (left, 0, (0, 0)))
    ):
        own = pl.ds(start, wide)
        size = reach * channels
        for which, (src, dst) in enumerate(
            (
                (atoms_ref.at[:, own], halo_x.at[side]),
                (cond_ref.at[own], halo_c.at[side]),
                (mask_ref, halo_m[side]),
                (token_ref, halo_t[side]),
                (
                    pair_ref.at[far[0], pl.ds(far[1], size)],
                    pair_far.at[pl.ds(skipped + side * size, size)],
                ),
            )
        ):
            copies.append(
                pltpu.make_async_remote_copy(
                    src_ref=src,
                    dst_ref=dst,
                    send_sem=send_sem.at[side, which],
                    recv_sem=recv_sem.at[side, which],
                    device_id={"atom": target},
                    device_id_type=MESH,
                )
            )
    to_right, to_left = copies[:5], copies[5:]

    def norm(values):
        values = values.astype(F32)
        centred = values - jnp.sum(values, axis=1, keepdims=True) * inverse
        spread = jnp.sum(centred * centred, axis=1, keepdims=True) * inverse
        return centred * lax.rsqrt(spread + EPS)

    @pl.when(has_left)
    def _():
        pl.semaphore_wait(barrier, 1)
        pl.semaphore_signal(ready_sem, inc=1, device_id={"atom": left}, device_id_type=MESH)

    for copy in loads[: len(early)]:
        copy.wait()

    @pl.when(has_left)
    def _():
        for copy in to_left:
            copy.start()

    own = pl.ds(0, atoms)
    factor = head_dim**-0.5

    def as_query(projected):
        return ((projected + query_bias_ref[...]) * factor).astype(BF16)

    def conditioning():
        cond_norm = norm(cond_ref[...]).astype(BF16)
        yield
        for which in range(2):
            adapt = mm(cond_norm, ada_ref[which])
            mod_ref[3 * which, own] = jax.nn.sigmoid(
                adapt[:, :width] + ada_bias_ref[which : which + 1]
            )
            mod_ref[3 * which + 1, own] = adapt[:, width:]
            yield
        zeroed = mm(cond_norm, jnp.concatenate([zero_ref[0], zero_ref[1]], axis=1))
        for which in range(2):
            mod_ref[3 * which + 2, own] = jax.nn.sigmoid(
                zeroed[:, which * width : (which + 1) * width] + zero_bias_ref[which : which + 1]
            )
        yield

    def projection(s):
        normed = norm(atoms_ref[s, own])
        yield
        attn_in = (normed * mod_ref[0, own] + mod_ref[1, own]).astype(BF16)
        projected = mm(attn_in, qkvg_ref[...])
        q_ref[s, own] = as_query(projected[:, :width])
        kv_ref[s, pl.ds(wide, atoms), pl.ds(0, 2 * width)] = projected[
            :, width : 3 * width
        ].astype(BF16)
        gate_ref[s, own] = jax.nn.sigmoid(projected[:, 3 * width :])
        yield

    starts = [conditioning(), projection(0), projection(1)]
    for stream in starts:
        next(stream)
    for stream in starts:
        for _ in stream:
            pass

    for copy in loads[len(early) :]:
        copy.wait()
    pair_copy.wait()

    weight = pair_weight_ref[...]
    weight = weight - jnp.mean(weight, axis=1, keepdims=True)
    spread_c = jnp.where(
        iota((channels, rows_half), 1) % channels == iota((channels, rows_half), 0), 1.0, 0.0
    ).astype(BF16)
    own_query = iota((half, rows_half), 1) // channels == iota((half, rows_half), 0)
    remaining = weight
    for piece in range(3):
        part = remaining.astype(BF16)
        remaining = remaining - part.astype(F32)
        broad = mm(part, spread_c)
        blocks = [
            jnp.where(own_query, jnp.broadcast_to(broad[h : h + 1], (half, rows_half)), 0.0)
            for h in range(heads)
        ]
        lhs_ref[pl.ds(rows_half + piece * lines, lines)] = jnp.concatenate(
            blocks, axis=0
        ).astype(BF16)

    def pair_window(w, block, keep):
        both = jnp.concatenate([block[:rows_half], block[rows_half:]], axis=1)
        result = mm(lhs_ref[...], both)
        square = None
        for c in range(channels):
            centred = result[c * half : (c + 1) * half]
            square = centred * centred if c == 0 else square + centred * centred
        at = rows_half
        total = (
            result[at : at + lines]
            + result[at + lines : at + 2 * lines]
            + result[at + 2 * lines : at + 3 * lines]
        )
        scale = lax.rsqrt(square * (1.0 / channels) + EPS)
        bias = total * jnp.concatenate([scale] * heads, axis=0)
        if keep is not None:
            bias = jnp.where(jnp.concatenate(keep, axis=1)[0:1] > 0.5, bias, DEAD)
        bias_ref[w, pl.ds(0, lines)] = bias[:, :key_len]
        bias_ref[w, pl.ds(lines, lines)] = bias[:, key_len:]

    def as_row(ref):
        return ref[...].reshape(1, atoms)

    def usable_at(mask, position):
        return (
            (mask == 1)
            & (position >= 0)
            & (position < n * atoms)
            & (position < count_ref[0])
        )

    def alive(usable):
        return jnp.broadcast_to(jnp.where(usable, 1.0, 0.0), (8, usable.shape[1]))

    def lanes_from(row, start, size):
        length = row.shape[1]
        return pltpu.roll(row, (length - start) % length, axis=1)[:, :size]

    inner = [
        w
        for w in range(windows)
        if w * query_len >= margin and w * query_len - margin + key_len <= atoms
    ]
    outer = [w for w in range(windows) if w not in inner]
    live = alive(usable_at(as_row(mask_ref), me * atoms + iota((1, atoms), 1)))
    def pairs():
        for w in inner:
            keep = lanes_from(live, w * query_len - margin, key_len)
            pair_window(w, pair_buf[w], [keep, keep])
            yield
        for w in outer:
            pair_window(w, pair_buf[w], None)
            yield

    head_of = iota((half, width), 1) // head_dim
    blank = jnp.zeros((key_len, width), BF16)

    def tiles_of(w, s):
        return [(t, (w + 1) * query_len, w * query_len, query_len, w, 0) for t in (s, s + 1)]

    def far_tiles(s):
        return [
            (s, 0, atoms, half, windows, 0),
            (s, atoms + 2 * wide - key_len, atoms + half, half, windows, lines),
        ]

    def stacked(s, row, count):
        query = q_ref[s, pl.ds(row, count)]
        parts = []
        for at in range(0, count, half):
            piece = query[at : at + half]
            for h in range(heads):
                parts.append(jnp.where(head_of == h, piece, jnp.zeros_like(piece)))
        return jnp.concatenate(parts, axis=0)

    def score(tiles):
        both = jnp.concatenate([stacked(s, row, m) for s, _, row, m, _, _ in tiles], axis=1)
        tall = []
        for s, key, _, _, _, _ in tiles:
            line = [blank] * len(tiles)
            line[len(tall)] = kv_ref[s, pl.ds(key, key_len), pl.ds(0, width)]
            tall.append(jnp.concatenate(line, axis=1))
        scores = lax.dot_general(
            both,
            jnp.concatenate(tall, axis=0),
            (((1,), (1,)), ((), ())),
            preferred_element_type=F32,
        )
        found = []
        for i, (_, _, _, m, w, line) in enumerate(tiles):
            own = scores[:, i * key_len : (i + 1) * key_len]
            own = own + bias_ref[w, pl.ds(line, heads * m)]
            found.append((own, jnp.max(own, axis=1, keepdims=True)))
        return found

    def mix(tiles, found):
        return [
            mm(
                jnp.exp(own - top).astype(BF16),
                kv_ref[s, pl.ds(key, key_len), pl.ds(width, 2 * width)],
            )
            for (s, key, _, _, _, _), (own, top) in zip(tiles, found)
        ]

    def blend(tiles, mixes):
        for (s, _, row, m, _, _), mixed in zip(tiles, mixes):
            rows = pl.ds(row, m)
            outs = []
            for base in range(0, heads * m, lines):
                value = mixed[base : base + half, :width]
                amount = mixed[base : base + half, width:]
                for h in range(1, heads):
                    at = base + h * half
                    value = jnp.where(head_of == h, mixed[at : at + half, :width], value)
                    amount = jnp.where(head_of == h, mixed[at : at + half, width:], amount)
                outs.append(value / amount)
            blend_ref[s, rows] = (jnp.concatenate(outs, axis=0) * gate_ref[s, rows]).astype(BF16)

    def transition(parts):
        def gather(ref):
            return jnp.concatenate([ref[s, pl.ds(a, m)] for s, a, m in parts], axis=0)

        def modulation(k):
            return jnp.concatenate([mod_ref[k, pl.ds(a, m)] for _, a, m in parts], axis=0)

        mixed = mm(gather(blend_ref), out_ref[...])
        yield
        after = (gather(atoms_ref).astype(F32) + modulation(2) * mixed).astype(BF16)
        trans_in = (norm(after) * modulation(3) + modulation(4)).astype(BF16)
        mixed = mm(trans_in, swiglu_ref[...])
        yield
        units = (jax.nn.silu(mixed[:, :hidden]) * mixed[:, hidden:]).astype(BF16)
        mixed = mm(units, down_ref[...])
        yield
        final = (after.astype(F32) + modulation(5) * mixed).astype(BF16)
        features = jnp.maximum(mm(final, token_weight_ref[...]), 0.0).astype(BF16)
        at = 0
        for s, a, m in parts:
            kept = min(a + m, atoms) - a
            atoms_out_ref[s, pl.ds(a, kept)] = final[at : at + kept]
            feat_ref[s, pl.ds(a, m)] = features[at : at + m]
            at += m
        yield

    def attention(units):
        found, mixes = {}, {}
        for i in range(len(units) + MIX_LAG + BLEND_LAG):
            if i < len(units):
                found[i] = score(units[i])
            j = i - MIX_LAG
            if 0 <= j < len(units):
                mixes[j] = mix(units[j], found.pop(j))
            j = j - BLEND_LAG
            if 0 <= j < len(units):
                blend(units[j], mixes.pop(j))
            yield

    def rotate(streams):
        streams = list(streams)
        while streams:
            for stream in list(streams):
                if next(stream, streams) is streams:
                    streams.remove(stream)
                else:
                    yield

    def series(*streams):
        for stream in streams:
            yield from stream

    def together(main, side, start, every):
        for i, _ in enumerate(main):
            if i >= start and (i - start) % every == 0:
                next(side, None)

    first, count = inner[0] * query_len, len(inner) * query_len
    bias_steps = pairs()
    together(bias_steps, series(projection(2), projection(3)), 1, 2)

    @pl.when(has_right)
    def _():
        pl.semaphore_wait(ready_sem, 1)
        for copy in to_right:
            copy.start()

    units = [tiles_of(w, s) for s in range(0, samples, 2) for w in inner]
    lag = MIX_LAG + BLEND_LAG
    fill = rotate([transition([(s, first, count)]) for s in range(2)])
    for i, _ in enumerate(attention(units)):
        if i >= len(inner) + lag:
            next(fill, None)
    fill = series(fill, rotate([transition([(s, first, count)]) for s in range(2, samples)]))
    for _ in range(AHEAD):
        next(fill, None)

    for to_there, out_there, in_there in (
        (to_right, has_right, has_left),
        (to_left, has_left, has_right),
    ):

        @pl.when(out_there)
        def _(copies=to_there):
            for copy in copies:
                copy.wait_send()

        @pl.when(in_there)
        def _(copies=to_there):
            for copy in copies:
                copy.wait_recv()

    extent = atoms + 2 * lanes

    def extended(halo, ref):
        return jnp.concatenate(
            [as_row(halo[0])[:, atoms - lanes :], as_row(ref), as_row(halo[1])[:, :lanes]],
            axis=1,
        )

    usable = usable_at(extended(halo_m, mask_ref), me * atoms - lanes + iota((1, extent), 1))
    relative = jnp.where(usable, extended(halo_t, token_ref) - me * tokens, -2)
    live = alive(usable)

    def halo():
        near = [pl.ds(wide - half, half), pl.ds(0, half)]
        for side in range(2):
            atoms_ref[:, pl.ds(atoms + side * half, half)] = halo_x[side, :, near[side]]
        cond_norm = norm(jnp.concatenate([halo_c[0], halo_c[1]], axis=0)).astype(BF16)
        normed = norm(
            jnp.concatenate(
                [halo_x[side].reshape(samples * wide, width) for side in range(2)], axis=0
            )
        ).reshape(2, samples, wide, width)
        adapt = mm(cond_norm, ada_ref[0])
        close = jnp.concatenate([cond_norm[wide - half : wide], cond_norm[wide : wide + half]], axis=0)
        close_adapt = mm(close, ada_ref[1])
        zeroed = mm(close, jnp.concatenate([zero_ref[0], zero_ref[1]], axis=1))
        far = [
            lanes_from(live, lanes - wide, key_len),
            lanes_from(live, lanes + atoms + wide - key_len, key_len),
        ]
        pair_window(windows, pair_far[...], far)
        yield
        for w in outer:
            keep = lanes_from(live, lanes + w * query_len - margin, key_len)[0:1] > 0.5
            bias_ref[w] = jnp.where(keep, bias_ref[w], DEAD)
        extra = pl.ds(atoms, 2 * half)
        mod_ref[3, extra] = jax.nn.sigmoid(close_adapt[:, :width] + ada_bias_ref[1:2])
        mod_ref[4, extra] = close_adapt[:, width:]
        for which in range(2):
            mod_ref[3 * which + 2, extra] = jax.nn.sigmoid(
                zeroed[:, which * width : (which + 1) * width] + zero_bias_ref[which : which + 1]
            )
        scale = jax.nn.sigmoid(adapt[:, :width] + ada_bias_ref[0:1])
        attn_in = (
            normed * scale.reshape(2, 1, wide, width)
            + adapt[:, width:].reshape(2, 1, wide, width)
        ).astype(BF16)
        projected = mm(
            attn_in.reshape(2 * samples * wide, width), qkvg_ref[:, pl.ds(width, 2 * width)]
        )
        close = jnp.concatenate(
            [
                attn_in[side, s, at : at + half]
                for s in range(samples)
                for side, at in enumerate((wide - half, 0))
            ],
            axis=0,
        )
        sides = mm(
            close,
            jnp.concatenate(
                [qkvg_ref[:, pl.ds(0, width)], qkvg_ref[:, pl.ds(3 * width, width)]], axis=1
            ),
        ).reshape(samples, 2 * half, 2 * width)
        yield
        for side, there in enumerate((has_left, has_right)):
            own = projected[side * samples * wide : (side + 1) * samples * wide]
            own = jnp.where(there, own, 0.0).astype(BF16)
            start = side * (wide + atoms)
            kv_ref[:, pl.ds(start, wide), pl.ds(0, 2 * width)] = own.reshape(
                samples, wide, 2 * width
            )
        for s in range(samples):
            q_ref[s, extra] = as_query(sides[s, :, :width])
            gate_ref[s, extra] = jax.nn.sigmoid(sides[s, :, width:])
        yield

    strip = iota((1, extent), 1)
    beyond = jnp.where(
        strip < half,
        pltpu.roll(jnp.broadcast_to(relative, (8, extent)), extent - lanes + half, axis=1)[0:1],
        pltpu.roll(jnp.broadcast_to(relative, (8, extent)), extent - lanes - atoms + half, axis=1)[0:1],
    )[:, : 2 * half]
    chosen = jnp.concatenate([relative[:, lanes : lanes + atoms], beyond], axis=1)
    total_atoms = atoms + 2 * half
    hits = iota((tokens, extent), 0) == jnp.broadcast_to(relative, (tokens, extent))
    per_count = 1.0 / jnp.maximum(
        jnp.sum(jnp.where(hits, 1.0, 0.0), axis=1, keepdims=True), 1.0
    )
    onehot = jnp.where(
        iota((tokens, total_atoms), 0) == jnp.broadcast_to(chosen, (tokens, total_atoms)), 1.0, 0.0
    ).astype(BF16)

    def closing(s):
        yield from transition(
            [(s, 0, first), (s, first + count, atoms - first - count + 2 * half)]
        )
        tokens_out_ref[s] = (mm(onehot, feat_ref[s]) * per_count).astype(BF16)
        yield

    for _ in halo():
        for _ in range(FILL_HALO):
            next(fill, None)
    units = []
    for s in range(0, samples, 2):
        units += [tiles_of(w, s) for w in outer] + [far_tiles(s), far_tiles(s + 1)]
    ready = len(units) // 2 + MIX_LAG + BLEND_LAG
    begun = rotate([closing(s) for s in range(samples // 2)])
    for i, _ in enumerate(attention(units)):
        if i >= ready:
            next(begun, None)
        elif i % FILL_EVERY == 0:
            next(fill, None)
    for _ in rotate([begun, fill] + [closing(s) for s in range(samples // 2, samples)]):
        pass


def on_device(
    n,
    atoms_in, cond, pair, atom_mask, atom_count, atom_to_token, ada_weight, ada_bias,
    zero_weight, zero_bias, qkvg_weight, query_bias, pair_weight, out_weight,
    swiglu_weight, down_weight, token_weight,
):
    samples, atoms, width = atoms_in.shape
    windows, query_len, channels, key_len = pair.shape
    heads = pair_weight.shape[0]
    wide = (key_len + query_len) // 2
    spread = atoms + query_len
    tokens = atoms // ATOMS_PER_TOKEN
    token_width = token_weight.shape[1]
    half = query_len // 2
    rows_half = half * channels
    vmem = pl.BlockSpec(memory_space=pltpu.VMEM)
    hbm = pl.BlockSpec(memory_space=pltpu.HBM)
    query_bias = query_bias.reshape(1, width)
    staged = (
        cond, ada_weight, ada_bias, zero_weight, zero_bias, qkvg_weight,
        query_bias, pair_weight, out_weight, swiglu_weight, down_weight, token_weight,
        atom_mask, atom_to_token,
    )
    return pl.pallas_call(
        functools.partial(block_body, n),
        out_shape=(
            pltpu.VMEM(atoms_in.shape, BF16),
            pltpu.VMEM((samples, tokens, token_width), BF16),
        ),
        in_specs=[hbm] * 17,
        out_specs=(vmem, vmem),
        scratch_shapes=[pltpu.VMEM(a.shape, a.dtype) for a in staged]
        + [
            pltpu.SMEM(atom_count.shape, atom_count.dtype),
            pltpu.VMEM((samples, spread, width), BF16),
            pltpu.VMEM((windows, query_len * channels, key_len), BF16),
            pltpu.VMEM((query_len * channels, key_len), BF16),
            pltpu.VMEM((2, samples, wide, width), BF16),
            pltpu.VMEM((2, wide, width), BF16),
            pltpu.VMEM((atoms,), jnp.int32),
            pltpu.VMEM((atoms,), jnp.int32),
            pltpu.VMEM((atoms,), jnp.int32),
            pltpu.VMEM((atoms,), jnp.int32),
            pltpu.VMEM((samples, atoms + 2 * wide, 3 * width), BF16),
            pltpu.VMEM((samples, spread, width), BF16),
            pltpu.VMEM((samples, spread, width), F32),
            pltpu.VMEM((windows + 1, heads * query_len, key_len), F32),
            pltpu.VMEM((6, spread, width), F32),
            pltpu.VMEM((samples, spread, token_width), BF16),
            pltpu.VMEM((samples, spread, width), BF16),
            pltpu.VMEM((rows_half + 3 * heads * half, rows_half), BF16),
            pltpu.SemaphoreType.DMA((len(staged) + 2,)),
            pltpu.SemaphoreType.DMA((1,)),
            pltpu.SemaphoreType.DMA((2, 5)),
            pltpu.SemaphoreType.DMA((2, 5)),
            pltpu.SemaphoreType.REGULAR,
        ],
        compiler_params=pltpu.CompilerParams(collective_id=0, has_side_effects=True),
        name="atom_block",
    )(
        atoms_in, cond, pair.reshape(windows, query_len * channels, key_len),
        atom_mask, atom_to_token, atom_count,
        ada_weight, ada_bias, zero_weight, zero_bias, qkvg_weight,
        query_bias, pair_weight, out_weight, swiglu_weight,
        down_weight, token_weight,
    )


def solution(mesh):
    shard = P(("struct", "atom"))
    stream = P("struct", "atom", None)
    in_specs = (stream, shard, shard, shard, P("struct"), shard) + (P(),) * 11
    return jax.shard_map(
        functools.partial(on_device, mesh.shape["atom"]),
        mesh=mesh,
        in_specs=in_specs,
        out_specs=(stream, stream),
        check_vma=False,
    )
```

```python
import functools

import jax
import jax.numpy as jnp
from jax import lax
from jax.experimental import pallas as pl
from jax.experimental.pallas import tpu as pltpu
from jax.sharding import PartitionSpec as P

ATOMS_PER_TOKEN = 8
EPS = 1e-05
DEAD = -1e30
MIX_LAG = 4
BLEND_LAG = 1
AHEAD = 0
T_LATE = 2
FILL_HALO = 3
FILL_EVERY = 2
MESH = pl.DeviceIdType.MESH
F32 = jnp.float32
BF16 = jnp.bfloat16


def iota(shape, axis):
    return lax.broadcasted_iota(jnp.int32, shape, axis)


def mm(a, b):
    return jnp.dot(a, b, preferred_element_type=F32)


def block_body(
    n,
    atoms_hbm, cond_hbm, pair_ref, mask_hbm, token_hbm, count_ref,
    ada_hbm, ada_bias_hbm, zero_hbm, zero_bias_hbm, qkvg_hbm, query_bias_hbm,
    pair_weight_hbm, out_hbm, swiglu_hbm, down_hbm, token_weight_hbm,
    atoms_out_ref, tokens_out_ref,
    cond_ref, ada_ref, ada_bias_ref, zero_ref, zero_bias_ref, qkvg_ref,
    query_bias_ref, pair_weight_ref, out_ref, swiglu_ref, down_ref, token_weight_ref,
    mask_ref, token_ref, atoms_ref,
    pair_buf, pair_far, halo_x, halo_c, halo_m0, halo_m1, halo_t0, halo_t1,
    keys_ref, values_ref, q_ref, gate_ref, bias_ref, mod_ref, feat_ref, blend_ref, lhs_ref,
    load_sem, pair_sem, send_sem, recv_sem, ready_sem,
):
    samples, atoms, width = atoms_out_ref.shape
    windows, rows_pair, key_len = pair_ref.shape
    heads, channels = pair_weight_ref.shape
    head_dim = width // heads
    query_len = rows_pair // channels
    half = query_len // 2
    margin = (key_len - query_len) // 2
    wide = margin + query_len
    reach = ATOMS_PER_TOKEN
    tokens = tokens_out_ref.shape[1]
    hidden = down_ref.shape[0]
    rows_half = half * channels
    lines = heads * half
    lanes = 128

    halo_m, halo_t = (halo_m0, halo_m1), (halo_t0, halo_t1)
    me = lax.axis_index("atom")
    right, left = lax.rem(me + 1, n), lax.rem(me + n - 1, n)

    barrier = pltpu.get_barrier_semaphore()
    has_left, has_right = me > 0, me < n - 1

    @pl.when(has_right)
    def _():
        pl.semaphore_signal(barrier, inc=1, device_id={"atom": right}, device_id_type=MESH)


    pair_copy = pltpu.make_async_copy(pair_ref, pair_buf, pair_sem.at[0])
    early = (
        (atoms_hbm, atoms_ref.at[:, pl.ds(0, atoms)]), (cond_hbm, cond_ref),
        (mask_hbm, mask_ref), (token_hbm, token_ref), (ada_hbm, ada_ref),
        (ada_bias_hbm, ada_bias_ref), (zero_hbm, zero_ref), (zero_bias_hbm, zero_bias_ref),
        (qkvg_hbm, qkvg_ref), (query_bias_hbm, query_bias_ref),
        (pair_weight_hbm, pair_weight_ref),
    )
    late = (
        (out_hbm, out_ref), (swiglu_hbm, swiglu_ref), (down_hbm, down_ref),
        (token_weight_hbm, token_weight_ref),
    )
    loads = [
        pltpu.make_async_copy(src, dst, load_sem.at[i])
        for i, (src, dst) in enumerate(early + late)
    ]
    for copy in loads[: len(early)]:
        copy.start()
    pair_copy.start()
    for copy in loads[len(early) :]:
        copy.start()

    inverse = 1.0 / width
    values_ref[:, :, width:] = jnp.ones((samples, atoms + 2 * key_len, width), BF16)
    row, col = iota((rows_half, rows_half), 0), iota((rows_half, rows_half), 1)
    place = (row % half) * channels + row // half
    same = jnp.where(row % half == col // channels, 1.0 / channels, 0.0)
    lhs_ref[pl.ds(0, rows_half)] = (jnp.where(place == col, 1.0, 0.0) - same).astype(BF16)

    skipped = rows_half - reach * channels
    pair_far[pl.ds(0, skipped)] = jnp.zeros((skipped, key_len), BF16)
    pair_far[pl.ds(2 * rows_half - skipped, skipped)] = jnp.zeros((skipped, key_len), BF16)
    for side, there in enumerate((has_left, has_right)):

        @pl.when(jnp.logical_not(there))
        def _(side=side):
            at = skipped + side * reach * channels
            pair_far[pl.ds(at, reach * channels)] = jnp.zeros((reach * channels, key_len), BF16)
            halo_x[side] = jnp.zeros(halo_x.shape[1:], BF16)
            halo_c[side] = jnp.zeros(halo_c.shape[1:], BF16)
            halo_m[side][...] = jnp.zeros(halo_m0.shape, jnp.int32)
            halo_t[side][...] = jnp.zeros(halo_t0.shape, jnp.int32)

    copies = []
    for side, (target, start, far) in enumerate(
        ((right, atoms - wide, (windows - 1, rows_pair - reach * channels)), (left, 0, (0, 0)))
    ):
        own = pl.ds(start, wide)
        size = reach * channels
        for which, (src, dst) in enumerate(
            (
                (atoms_ref.at[:, own], halo_x.at[side]),
                (cond_ref.at[own], halo_c.at[side]),
                (mask_ref, halo_m[side]),
                (token_ref, halo_t[side]),
                (
                    pair_ref.at[far[0], pl.ds(far[1], size)],
                    pair_far.at[pl.ds(skipped + side * size, size)],
                ),
            )
        ):
            copies.append(
                pltpu.make_async_remote_copy(
                    src_ref=src,
                    dst_ref=dst,
                    send_sem=send_sem.at[side, which],
                    recv_sem=recv_sem.at[side, which],
                    device_id={"atom": target},
                    device_id_type=MESH,
                )
            )
    to_right, to_left = copies[:5], copies[5:]

    def norm(values):
        values = values.astype(F32)
        centred = values - jnp.sum(values, axis=1, keepdims=True) * inverse
        spread = jnp.sum(centred * centred, axis=1, keepdims=True) * inverse
        return centred * lax.rsqrt(spread + EPS)

    @pl.when(has_left)
    def _():
        pl.semaphore_wait(barrier, 1)
        pl.semaphore_signal(ready_sem, inc=1, device_id={"atom": left}, device_id_type=MESH)

    for copy in loads[:4]:
        copy.wait()

    @pl.when(has_left)
    def _():
        for copy in to_left:
            copy.start()

    for copy in loads[4 : len(early)]:
        copy.wait()

    own = pl.ds(0, atoms)
    factor = head_dim**-0.5

    def as_query(projected):
        return ((projected + query_bias_ref[...]) * factor).astype(BF16)

    def conditioning():
        cond_norm = norm(cond_ref[...]).astype(BF16)
        yield
        for which in range(2):
            adapt = mm(cond_norm, ada_ref[which])
            mod_ref[3 * which, own] = jax.nn.sigmoid(
                adapt[:, :width] + ada_bias_ref[which : which + 1]
            )
            mod_ref[3 * which + 1, own] = adapt[:, width:]
            yield
        zeroed = mm(cond_norm, jnp.concatenate([zero_ref[0], zero_ref[1]], axis=1))
        for which in range(2):
            mod_ref[3 * which + 2, own] = jax.nn.sigmoid(
                zeroed[:, which * width : (which + 1) * width] + zero_bias_ref[which : which + 1]
            )
        yield

    def projection(s):
        normed = norm(atoms_ref[s, own])
        yield
        attn_in = (normed * mod_ref[0, own] + mod_ref[1, own]).astype(BF16)
        projected = mm(attn_in, qkvg_ref[...])
        q_ref[s, own] = as_query(projected[:, :width])
        key = projected[:, width : 2 * width].astype(BF16)
        for t in range(atoms // key_len):
            keys_ref[s, t + 1] = key[t * key_len : (t + 1) * key_len].T
        values_ref[s, pl.ds(key_len, atoms), pl.ds(0, width)] = projected[
            :, 2 * width : 3 * width
        ].astype(BF16)
        gate_ref[s, own] = jax.nn.sigmoid(projected[:, 3 * width :])
        yield

    starts = [conditioning(), projection(0), projection(1)]
    for stream in starts:
        next(stream)
    for stream in starts:
        for _ in stream:
            pass

    @pl.when(has_right)
    def _():
        pl.semaphore_wait(ready_sem, 1)
        for copy in to_right:
            copy.start()

    for copy in loads[len(early) :]:
        copy.wait()
    pair_copy.wait()

    weight = pair_weight_ref[...]
    weight = weight - jnp.mean(weight, axis=1, keepdims=True)
    spread_c = jnp.where(
        iota((channels, rows_half), 1) % channels == iota((channels, rows_half), 0), 1.0, 0.0
    ).astype(BF16)
    own_query = iota((half, rows_half), 1) // channels == iota((half, rows_half), 0)
    remaining = weight
    for piece in range(3):
        part = remaining.astype(BF16)
        remaining = remaining - part.astype(F32)
        broad = mm(part, spread_c)
        blocks = [
            jnp.where(own_query, jnp.broadcast_to(broad[h : h + 1], (half, rows_half)), 0.0)
            for h in range(heads)
        ]
        lhs_ref[pl.ds(rows_half + piece * lines, lines)] = jnp.concatenate(
            blocks, axis=0
        ).astype(BF16)

    def turned(bias, start):
        turn = start % key_len
        return pltpu.roll(bias, turn, axis=1) if turn else bias

    def pair_window(w, block, keep, starts):
        both = jnp.concatenate([block[:rows_half], block[rows_half:]], axis=1)
        result = mm(lhs_ref[...], both)
        square = None
        for c in range(channels):
            centred = result[c * half : (c + 1) * half]
            square = centred * centred if c == 0 else square + centred * centred
        at = rows_half
        total = (
            result[at : at + lines]
            + result[at + lines : at + 2 * lines]
            + result[at + 2 * lines : at + 3 * lines]
        )
        scale = lax.rsqrt(square * (1.0 / channels) + EPS)
        bias = total * jnp.concatenate([scale] * heads, axis=0)
        if keep is not None:
            bias = jnp.where(jnp.concatenate(keep, axis=1)[0:1] > 0.5, bias, DEAD)
        bias_ref[w, pl.ds(0, lines)] = turned(bias[:, :key_len], starts[0])
        bias_ref[w, pl.ds(lines, lines)] = turned(bias[:, key_len:], starts[1])

    def as_row(ref):
        return ref[...].reshape(1, atoms)

    def usable_at(mask, position):
        return (
            (mask == 1)
            & (position >= 0)
            & (position < n * atoms)
            & (position < count_ref[0])
        )

    def alive(usable):
        return jnp.broadcast_to(jnp.where(usable, 1.0, 0.0), (8, usable.shape[1]))

    def lanes_from(row, start, size):
        length = row.shape[1]
        return pltpu.roll(row, (length - start) % length, axis=1)[:, :size]

    inner = [
        w
        for w in range(windows)
        if w * query_len >= margin and w * query_len - margin + key_len <= atoms
    ]
    outer = [w for w in range(windows) if w not in inner]
    live = alive(usable_at(as_row(mask_ref), me * atoms + iota((1, atoms), 1)))
    def first_key(w):
        return key_len + w * query_len - margin

    far_keys = (key_len - wide, key_len + atoms + wide - key_len)

    def pairs():
        for w in inner:
            keep = lanes_from(live, w * query_len - margin, key_len)
            pair_window(w, pair_buf[w], [keep, keep], [first_key(w)] * 2)
            yield
        for w in outer:
            pair_window(w, pair_buf[w], None, [first_key(w)] * 2)
            yield

    head_of = iota((half, width), 1) // head_dim
    blank = jnp.zeros((width, key_len), BF16)
    lane = iota((width, key_len), 1)

    def tiles_of(w, s):
        return [(t, first_key(w), w * query_len, query_len, w, 0) for t in (s, s + 1)]

    def far_tiles(s):
        return [
            (s, far_keys[0], atoms, half, windows, 0),
            (s, far_keys[1], atoms + half, half, windows, lines),
        ]

    def stacked(s, row, count):
        query = q_ref[s, pl.ds(row, count)]
        parts = []
        for at in range(0, count, half):
            piece = query[at : at + half]
            for h in range(heads):
                parts.append(jnp.where(head_of == h, piece, jnp.zeros_like(piece)))
        return jnp.concatenate(parts, axis=0)

    def score(tiles):
        both = jnp.concatenate([stacked(s, row, m) for s, _, row, m, _, _ in tiles], axis=1)
        tall = []
        for s, key, _, _, _, _ in tiles:
            line = [blank] * len(tiles)
            t, turn = key // key_len, key % key_len
            line[len(tall)] = jnp.where(lane < turn, keys_ref[s, t + 1], keys_ref[s, t])
            tall.append(jnp.concatenate(line, axis=1))
        scores = mm(both, jnp.concatenate(tall, axis=0))
        found = []
        for i, (_, _, _, m, w, line) in enumerate(tiles):
            own = scores[:, i * key_len : (i + 1) * key_len]
            own = own + bias_ref[w, pl.ds(line, heads * m)]
            found.append((own, jnp.max(own, axis=1, keepdims=True)))
        return found

    def mix(tiles, found):
        mixes = []
        for (s, key, _, _, _, _), (own, top) in zip(tiles, found):
            turn = key % key_len
            split = key + key_len - turn
            value = values_ref[s, pl.ds(key, key_len - turn)]
            if turn:
                value = jnp.concatenate([values_ref[s, pl.ds(split, turn)], value], axis=0)
            mixes.append(mm(jnp.exp(own - top).astype(BF16), value))
        return mixes

    def blend(tiles, mixes):
        for (s, _, row, m, _, _), mixed in zip(tiles, mixes):
            rows = pl.ds(row, m)
            outs = []
            for base in range(0, heads * m, lines):
                value = mixed[base : base + half, :width]
                amount = mixed[base : base + half, width:]
                for h in range(1, heads):
                    at = base + h * half
                    value = jnp.where(head_of == h, mixed[at : at + half, :width], value)
                    amount = jnp.where(head_of == h, mixed[at : at + half, width:], amount)
                outs.append(value / amount)
            blend_ref[s, rows] = (jnp.concatenate(outs, axis=0) * gate_ref[s, rows]).astype(BF16)

    def transition(parts):
        def gather(ref):
            return jnp.concatenate([ref[s, pl.ds(a, m)] for s, a, m in parts], axis=0)

        def modulation(k):
            return jnp.concatenate([mod_ref[k, pl.ds(a, m)] for _, a, m in parts], axis=0)

        mixed = mm(gather(blend_ref), out_ref[...])
        yield
        after = (gather(atoms_ref).astype(F32) + modulation(2) * mixed).astype(BF16)
        trans_in = (norm(after) * modulation(3) + modulation(4)).astype(BF16)
        mixed = mm(trans_in, swiglu_ref[...])
        yield
        units = (jax.nn.silu(mixed[:, :hidden]) * mixed[:, hidden:]).astype(BF16)
        mixed = mm(units, down_ref[...])
        yield
        final = (after.astype(F32) + modulation(5) * mixed).astype(BF16)
        features = jnp.maximum(mm(final, token_weight_ref[...]), 0.0).astype(BF16)
        at = 0
        for s, a, m in parts:
            kept = min(a + m, atoms) - a
            atoms_out_ref[s, pl.ds(a, kept)] = final[at : at + kept]
            feat_ref[s, pl.ds(a, m)] = features[at : at + m]
            at += m
        yield

    def attention(units):
        found, mixes = {}, {}
        for i in range(len(units) + MIX_LAG + BLEND_LAG):
            if i < len(units):
                found[i] = score(units[i])
            j = i - MIX_LAG
            if 0 <= j < len(units):
                mixes[j] = mix(units[j], found.pop(j))
            j = j - BLEND_LAG
            if 0 <= j < len(units):
                blend(units[j], mixes.pop(j))
            yield

    def rotate(streams):
        streams = list(streams)
        while streams:
            for stream in list(streams):
                if next(stream, streams) is streams:
                    streams.remove(stream)
                else:
                    yield

    def series(*streams):
        for stream in streams:
            yield from stream

    def together(main, side, start, every):
        for i, _ in enumerate(main):
            if i >= start and (i - start) % every == 0:
                next(side, None)

    first, count = inner[0] * query_len, len(inner) * query_len
    bias_steps = pairs()
    together(bias_steps, series(projection(2), projection(3)), 1, 2)

    units = [tiles_of(w, s) for s in range(0, samples, 2) for w in inner]
    lag = MIX_LAG + BLEND_LAG
    fill = rotate([transition([(s, first, count)]) for s in range(2)])
    for i, _ in enumerate(attention(units)):
        if i >= len(inner) + lag + T_LATE:
            next(fill, None)
    fill = series(fill, rotate([transition([(s, first, count)]) for s in range(2, samples)]))
    for _ in range(AHEAD):
        next(fill, None)

    for to_there, out_there, in_there in (
        (to_right, has_right, has_left),
        (to_left, has_left, has_right),
    ):

        @pl.when(out_there)
        def _(copies=to_there):
            for copy in copies:
                copy.wait_send()

        @pl.when(in_there)
        def _(copies=to_there):
            for copy in copies:
                copy.wait_recv()

    extent = atoms + 2 * lanes

    def extended(halo, ref):
        return jnp.concatenate(
            [as_row(halo[0])[:, atoms - lanes :], as_row(ref), as_row(halo[1])[:, :lanes]],
            axis=1,
        )

    usable = usable_at(extended(halo_m, mask_ref), me * atoms - lanes + iota((1, extent), 1))
    relative = jnp.where(usable, extended(halo_t, token_ref) - me * tokens, -2)
    live = alive(usable)

    def halo():
        near = [pl.ds(wide - half, half), pl.ds(0, half)]
        for side in range(2):
            atoms_ref[:, pl.ds(atoms + side * half, half)] = halo_x[side, :, near[side]]
        cond_norm = norm(jnp.concatenate([halo_c[0], halo_c[1]], axis=0)).astype(BF16)
        normed = norm(
            jnp.concatenate(
                [halo_x[side].reshape(samples * wide, width) for side in range(2)], axis=0
            )
        ).reshape(2, samples, wide, width)
        adapt = mm(cond_norm, ada_ref[0])
        close = jnp.concatenate([cond_norm[wide - half : wide], cond_norm[wide : wide + half]], axis=0)
        close_adapt = mm(close, ada_ref[1])
        zeroed = mm(close, jnp.concatenate([zero_ref[0], zero_ref[1]], axis=1))
        far = [
            lanes_from(live, lanes - wide, key_len),
            lanes_from(live, lanes + atoms + wide - key_len, key_len),
        ]
        pair_window(windows, pair_far[...], far, far_keys)
        yield
        for w in outer:
            keep = lanes_from(live, lanes + w * query_len - margin, key_len)
            keep = turned(keep, first_key(w))[0:1] > 0.5
            bias_ref[w] = jnp.where(keep, bias_ref[w], DEAD)
        extra = pl.ds(atoms, 2 * half)
        mod_ref[3, extra] = jax.nn.sigmoid(close_adapt[:, :width] + ada_bias_ref[1:2])
        mod_ref[4, extra] = close_adapt[:, width:]
        for which in range(2):
            mod_ref[3 * which + 2, extra] = jax.nn.sigmoid(
                zeroed[:, which * width : (which + 1) * width] + zero_bias_ref[which : which + 1]
            )
        scale = jax.nn.sigmoid(adapt[:, :width] + ada_bias_ref[0:1])
        attn_in = (
            normed * scale.reshape(2, 1, wide, width)
            + adapt[:, width:].reshape(2, 1, wide, width)
        ).astype(BF16)
        projected = mm(
            attn_in.reshape(2 * samples * wide, width), qkvg_ref[:, pl.ds(width, 2 * width)]
        )
        close = jnp.concatenate(
            [
                attn_in[side, s, at : at + half]
                for s in range(samples)
                for side, at in enumerate((wide - half, 0))
            ],
            axis=0,
        )
        sides = mm(
            close,
            jnp.concatenate(
                [qkvg_ref[:, pl.ds(0, width)], qkvg_ref[:, pl.ds(3 * width, width)]], axis=1
            ),
        ).reshape(samples, 2 * half, 2 * width)
        yield
        for side, there in enumerate((has_left, has_right)):
            own = projected[side * samples * wide : (side + 1) * samples * wide]
            own = jnp.where(there, own, 0.0).astype(BF16).reshape(samples, wide, 2 * width)
            start = key_len - wide if side == 0 else key_len + atoms
            values_ref[:, pl.ds(start, wide), pl.ds(0, width)] = own[:, :, width:]
            rest = jnp.zeros((key_len - wide, width), BF16)
            for s in range(samples):
                key = own[s, :, :width]
                key = [rest, key] if side == 0 else [key, rest]
                tile = 0 if side == 0 else atoms // key_len + 1
                keys_ref[s, tile] = jnp.concatenate(key, axis=0).T
        for s in range(samples):
            q_ref[s, extra] = as_query(sides[s, :, :width])
            gate_ref[s, extra] = jax.nn.sigmoid(sides[s, :, width:])
        yield

    strip = iota((1, extent), 1)
    beyond = jnp.where(
        strip < half,
        pltpu.roll(jnp.broadcast_to(relative, (8, extent)), extent - lanes + half, axis=1)[0:1],
        pltpu.roll(jnp.broadcast_to(relative, (8, extent)), extent - lanes - atoms + half, axis=1)[0:1],
    )[:, : 2 * half]
    chosen = jnp.concatenate([relative[:, lanes : lanes + atoms], beyond], axis=1)
    total_atoms = atoms + 2 * half
    hits = iota((tokens, extent), 0) == jnp.broadcast_to(relative, (tokens, extent))
    per_count = 1.0 / jnp.maximum(
        jnp.sum(jnp.where(hits, 1.0, 0.0), axis=1, keepdims=True), 1.0
    )
    onehot = jnp.where(
        iota((tokens, total_atoms), 0) == jnp.broadcast_to(chosen, (tokens, total_atoms)), 1.0, 0.0
    ).astype(BF16)

    def closing(s):
        yield from transition(
            [(s, 0, first), (s, first + count, atoms - first - count + 2 * half)]
        )
        tokens_out_ref[s] = (mm(onehot, feat_ref[s]) * per_count).astype(BF16)
        yield

    for _ in halo():
        for _ in range(FILL_HALO):
            next(fill, None)
    units = []
    for s in range(0, samples, 2):
        units += [tiles_of(w, s) for w in outer] + [far_tiles(s), far_tiles(s + 1)]
    ready = len(units) // 2 + MIX_LAG + BLEND_LAG
    begun = rotate([closing(s) for s in range(samples // 2)])
    for i, _ in enumerate(attention(units)):
        if i >= ready:
            next(begun, None)
        elif i % FILL_EVERY == 0:
            next(fill, None)
    for _ in rotate([begun, fill] + [closing(s) for s in range(samples // 2, samples)]):
        pass


def flush_body(atoms_ref, tokens_ref, atoms_out_ref, tokens_out_ref, sem):
    copies = [
        pltpu.make_async_copy(atoms_ref, atoms_out_ref, sem.at[0]),
        pltpu.make_async_copy(tokens_ref, tokens_out_ref, sem.at[1]),
    ]
    for copy in copies:
        copy.start()
    for copy in copies:
        copy.wait()


def on_device(
    n,
    atoms_in, cond, pair, atom_mask, atom_count, atom_to_token, ada_weight, ada_bias,
    zero_weight, zero_bias, qkvg_weight, query_bias, pair_weight, out_weight,
    swiglu_weight, down_weight, token_weight,
):
    samples, atoms, width = atoms_in.shape
    windows, query_len, channels, key_len = pair.shape
    heads = pair_weight.shape[0]
    wide = (key_len + query_len) // 2
    spread = atoms + query_len
    tokens = atoms // ATOMS_PER_TOKEN
    token_width = token_weight.shape[1]
    half = query_len // 2
    rows_half = half * channels
    vmem = pl.BlockSpec(memory_space=pltpu.VMEM)
    hbm = pl.BlockSpec(memory_space=pltpu.HBM)
    query_bias = query_bias.reshape(1, width)
    staged = (
        cond, ada_weight, ada_bias, zero_weight, zero_bias, qkvg_weight,
        query_bias, pair_weight, out_weight, swiglu_weight, down_weight, token_weight,
        atom_mask, atom_to_token,
    )
    held = pl.pallas_call(
        functools.partial(block_body, n),
        out_shape=(
            pltpu.VMEM(atoms_in.shape, BF16),
            pltpu.VMEM((samples, tokens, token_width), BF16),
        ),
        in_specs=[hbm] * 5 + [pl.BlockSpec(memory_space=pltpu.SMEM)] + [hbm] * 11,
        out_specs=(vmem, vmem),
        scratch_shapes=[pltpu.VMEM(a.shape, a.dtype) for a in staged]
        + [
            pltpu.VMEM((samples, spread, width), BF16),
            pltpu.VMEM((windows, query_len * channels, key_len), BF16),
            pltpu.VMEM((query_len * channels, key_len), BF16),
            pltpu.VMEM((2, samples, wide, width), BF16),
            pltpu.VMEM((2, wide, width), BF16),
            pltpu.VMEM((atoms,), jnp.int32),
            pltpu.VMEM((atoms,), jnp.int32),
            pltpu.VMEM((atoms,), jnp.int32),
            pltpu.VMEM((atoms,), jnp.int32),
            pltpu.VMEM((samples, atoms // key_len + 2, width, key_len), BF16),
            pltpu.VMEM((samples, atoms + 2 * key_len, 2 * width), BF16),
            pltpu.VMEM((samples, spread, width), BF16),
            pltpu.VMEM((samples, spread, width), F32),
            pltpu.VMEM((windows + 1, heads * query_len, key_len), F32),
            pltpu.VMEM((6, spread, width), F32),
            pltpu.VMEM((samples, spread, token_width), BF16),
            pltpu.VMEM((samples, spread, width), BF16),
            pltpu.VMEM((rows_half + 3 * heads * half, rows_half), BF16),
            pltpu.SemaphoreType.DMA((len(staged) + 1,)),
            pltpu.SemaphoreType.DMA((1,)),
            pltpu.SemaphoreType.DMA((2, 5)),
            pltpu.SemaphoreType.DMA((2, 5)),
            pltpu.SemaphoreType.REGULAR,
        ],
        compiler_params=pltpu.CompilerParams(collective_id=0, has_side_effects=True),
        name="atom_block",
    )(
        atoms_in, cond, pair.reshape(windows, query_len * channels, key_len),
        atom_mask, atom_to_token, atom_count,
        ada_weight, ada_bias, zero_weight, zero_bias, qkvg_weight,
        query_bias, pair_weight, out_weight, swiglu_weight,
        down_weight, token_weight,
    )
    return pl.pallas_call(
        flush_body,
        out_shape=tuple(jax.ShapeDtypeStruct(a.shape, a.dtype) for a in held),
        in_specs=[pl.BlockSpec(memory_space=pl.ANY)] * 2,
        out_specs=(hbm, hbm),
        scratch_shapes=[pltpu.SemaphoreType.DMA((2,))],
        name="flush",
    )(*[pltpu.with_memory_space_constraint(a, pltpu.VMEM) for a in held])


def solution(mesh):
    shard = P(("struct", "atom"))
    stream = P("struct", "atom", None)
    in_specs = (stream, shard, shard, shard, P("struct"), shard) + (P(),) * 11
    return jax.shard_map(
        functools.partial(on_device, mesh.shape["atom"]),
        mesh=mesh,
        in_specs=in_specs,
        out_specs=(stream, stream),
        check_vma=False,
    )
```

```python
import functools

import jax
import jax.numpy as jnp
from jax import lax
from jax.experimental import pallas as pl
from jax.experimental.pallas import tpu as pltpu
from jax.sharding import PartitionSpec as P

ATOMS_PER_TOKEN = 8
EPS = 1e-05
DEAD = -1e30
MIX_LAG = 4
BLEND_LAG = 1
AHEAD = 4
T_LATE = 0
FILL_HALO = 1
FILL_EVERY = 2
MESH = pl.DeviceIdType.MESH
F32 = jnp.float32
BF16 = jnp.bfloat16


def iota(shape, axis):
    return lax.broadcasted_iota(jnp.int32, shape, axis)


def mm(a, b):
    return jnp.dot(a, b, preferred_element_type=F32)


def block_body(
    n,
    atoms_hbm, cond_hbm, pair_ref, mask_hbm, token_hbm, count_ref,
    ada_hbm, ada_bias_hbm, zero_hbm, zero_bias_hbm, qkvg_hbm, query_bias_hbm,
    pair_weight_hbm, out_hbm, swiglu_hbm, down_hbm, token_weight_hbm,
    atoms_out_ref, tokens_out_ref,
    cond_ref, ada_ref, ada_bias_ref, zero_ref, zero_bias_ref, qkvg_ref,
    query_bias_ref, pair_weight_ref, out_ref, swiglu_ref, down_ref, token_weight_ref,
    mask_ref, token_ref, atoms_ref,
    lead_x, lead_c, pair_buf, pair_far, halo_x, halo_c, halo_m0, halo_m1, halo_t0, halo_t1,
    keys_ref, values_ref, q_ref, gate_ref, bias_ref, mod_ref, feat_ref, blend_ref, lhs_ref,
    load_sem, pair_sem, send_sem, recv_sem, ready_sem,
):
    samples, atoms, width = atoms_out_ref.shape
    windows, rows_pair, key_len = pair_ref.shape
    heads, channels = pair_weight_ref.shape
    head_dim = width // heads
    query_len = rows_pair // channels
    half = query_len // 2
    margin = (key_len - query_len) // 2
    wide = margin + query_len
    reach = ATOMS_PER_TOKEN
    tokens = tokens_out_ref.shape[1]
    hidden = down_ref.shape[0]
    rows_half = half * channels
    lines = heads * half
    lanes = 128

    halo_m, halo_t = (halo_m0, halo_m1), (halo_t0, halo_t1)
    me = lax.axis_index("atom")
    right, left = lax.rem(me + 1, n), lax.rem(me + n - 1, n)

    barrier = pltpu.get_barrier_semaphore()
    has_left, has_right = me > 0, me < n - 1

    @pl.when(has_right)
    def _():
        pl.semaphore_signal(barrier, inc=1, device_id={"atom": right}, device_id_type=MESH)


    pair_copy = pltpu.make_async_copy(pair_ref, pair_buf, pair_sem.at[0])
    early = (
        (atoms_hbm.at[:, pl.ds(0, wide)], lead_x), (cond_hbm.at[pl.ds(0, wide)], lead_c),
        (mask_hbm, mask_ref), (token_hbm, token_ref),
        (atoms_hbm, atoms_ref.at[:, pl.ds(0, atoms)]), (cond_hbm, cond_ref), (ada_hbm, ada_ref),
        (ada_bias_hbm, ada_bias_ref), (zero_hbm, zero_ref), (zero_bias_hbm, zero_bias_ref),
        (qkvg_hbm, qkvg_ref), (query_bias_hbm, query_bias_ref),
        (pair_weight_hbm, pair_weight_ref),
    )
    late = (
        (out_hbm, out_ref), (swiglu_hbm, swiglu_ref), (down_hbm, down_ref),
        (token_weight_hbm, token_weight_ref),
    )
    loads = [
        pltpu.make_async_copy(src, dst, load_sem.at[i])
        for i, (src, dst) in enumerate(early + late)
    ]
    for copy in loads[: len(early)]:
        copy.start()
    pair_copy.start()
    for copy in loads[len(early) :]:
        copy.start()

    inverse = 1.0 / width
    values_ref[:, :, width:] = jnp.ones((samples, atoms + 2 * key_len, width), BF16)
    row, col = iota((rows_half, rows_half), 0), iota((rows_half, rows_half), 1)
    place = (row % half) * channels + row // half
    same = jnp.where(row % half == col // channels, 1.0 / channels, 0.0)
    lhs_ref[pl.ds(0, rows_half)] = (jnp.where(place == col, 1.0, 0.0) - same).astype(BF16)

    skipped = rows_half - reach * channels
    pair_far[pl.ds(0, skipped)] = jnp.zeros((skipped, key_len), BF16)
    pair_far[pl.ds(2 * rows_half - skipped, skipped)] = jnp.zeros((skipped, key_len), BF16)
    for side, there in enumerate((has_left, has_right)):

        @pl.when(jnp.logical_not(there))
        def _(side=side):
            at = skipped + side * reach * channels
            pair_far[pl.ds(at, reach * channels)] = jnp.zeros((reach * channels, key_len), BF16)
            halo_x[side] = jnp.zeros(halo_x.shape[1:], BF16)
            halo_c[side] = jnp.zeros(halo_c.shape[1:], BF16)
            halo_m[side][...] = jnp.zeros(halo_m0.shape, jnp.int32)
            halo_t[side][...] = jnp.zeros(halo_t0.shape, jnp.int32)

    copies = []
    for side, (target, start, far) in enumerate(
        ((right, atoms - wide, (windows - 1, rows_pair - reach * channels)), (left, 0, (0, 0)))
    ):
        own = pl.ds(start, wide)
        size = reach * channels
        for which, (src, dst) in enumerate(
            (
                (lead_x if side else atoms_ref.at[:, own], halo_x.at[side]),
                (lead_c if side else cond_ref.at[own], halo_c.at[side]),
                (mask_ref, halo_m[side]),
                (token_ref, halo_t[side]),
                (
                    pair_ref.at[far[0], pl.ds(far[1], size)],
                    pair_far.at[pl.ds(skipped + side * size, size)],
                ),
            )
        ):
            copies.append(
                pltpu.make_async_remote_copy(
                    src_ref=src,
                    dst_ref=dst,
                    send_sem=send_sem.at[side, which],
                    recv_sem=recv_sem.at[side, which],
                    device_id={"atom": target},
                    device_id_type=MESH,
                )
            )
    to_right, to_left = copies[:5], copies[5:]

    def norm(values):
        values = values.astype(F32)
        centred = values - jnp.sum(values, axis=1, keepdims=True) * inverse
        spread = jnp.sum(centred * centred, axis=1, keepdims=True) * inverse
        return centred * lax.rsqrt(spread + EPS)

    @pl.when(has_left)
    def _():
        pl.semaphore_wait(barrier, 1)
        pl.semaphore_signal(ready_sem, inc=1, device_id={"atom": left}, device_id_type=MESH)

    for copy in loads[:4]:
        copy.wait()

    @pl.when(has_left)
    def _():
        for copy in to_left:
            copy.start()

    for copy in loads[4 : len(early)]:
        copy.wait()

    own = pl.ds(0, atoms)
    factor = head_dim**-0.5

    def as_query(projected):
        return ((projected + query_bias_ref[...]) * factor).astype(BF16)

    def conditioning():
        cond_norm = norm(cond_ref[...]).astype(BF16)
        yield
        for which in range(2):
            adapt = mm(cond_norm, ada_ref[which])
            mod_ref[3 * which, own] = jax.nn.sigmoid(
                adapt[:, :width] + ada_bias_ref[which : which + 1]
            )
            mod_ref[3 * which + 1, own] = adapt[:, width:]
            yield
        zeroed = mm(cond_norm, jnp.concatenate([zero_ref[0], zero_ref[1]], axis=1))
        for which in range(2):
            mod_ref[3 * which + 2, own] = jax.nn.sigmoid(
                zeroed[:, which * width : (which + 1) * width] + zero_bias_ref[which : which + 1]
            )
        yield

    def projection(s):
        normed = norm(atoms_ref[s, own])
        yield
        attn_in = (normed * mod_ref[0, own] + mod_ref[1, own]).astype(BF16)
        projected = mm(attn_in, qkvg_ref[...])
        q_ref[s, own] = as_query(projected[:, :width])
        key = projected[:, width : 2 * width].astype(BF16)
        for t in range(atoms // key_len):
            keys_ref[s, t + 1] = key[t * key_len : (t + 1) * key_len].T
        values_ref[s, pl.ds(key_len, atoms), pl.ds(0, width)] = projected[
            :, 2 * width : 3 * width
        ].astype(BF16)
        gate_ref[s, own] = jax.nn.sigmoid(projected[:, 3 * width :])
        yield

    starts = [conditioning(), projection(0), projection(1)]
    for stream in starts:
        next(stream)

    weight = pair_weight_ref[...]
    weight = weight - jnp.mean(weight, axis=1, keepdims=True)
    spread_c = jnp.where(
        iota((channels, rows_half), 1) % channels == iota((channels, rows_half), 0), 1.0, 0.0
    ).astype(BF16)
    own_query = iota((half, rows_half), 1) // channels == iota((half, rows_half), 0)
    remaining = weight
    for piece in range(3):
        part = remaining.astype(BF16)
        remaining = remaining - part.astype(F32)
        broad = mm(part, spread_c)
        blocks = [
            jnp.where(own_query, jnp.broadcast_to(broad[h : h + 1], (half, rows_half)), 0.0)
            for h in range(heads)
        ]
        lhs_ref[pl.ds(rows_half + piece * lines, lines)] = jnp.concatenate(
            blocks, axis=0
        ).astype(BF16)

    for stream in starts:
        for _ in stream:
            pass

    @pl.when(has_right)
    def _():
        pl.semaphore_wait(ready_sem, 1)
        for copy in to_right:
            copy.start()

    for copy in loads[len(early) :]:
        copy.wait()
    pair_copy.wait()

    def turned(bias, start):
        turn = start % key_len
        return pltpu.roll(bias, turn, axis=1) if turn else bias

    def pair_window(w, block, keep, starts):
        both = jnp.concatenate([block[:rows_half], block[rows_half:]], axis=1)
        result = mm(lhs_ref[...], both)
        square = None
        for c in range(channels):
            centred = result[c * half : (c + 1) * half]
            square = centred * centred if c == 0 else square + centred * centred
        at = rows_half
        total = (
            result[at : at + lines]
            + result[at + lines : at + 2 * lines]
            + result[at + 2 * lines : at + 3 * lines]
        )
        scale = lax.rsqrt(square * (1.0 / channels) + EPS)
        bias = total * jnp.concatenate([scale] * heads, axis=0)
        if keep is not None:
            bias = jnp.where(jnp.concatenate(keep, axis=1)[0:1] > 0.5, bias, DEAD)
        bias_ref[w, pl.ds(0, lines)] = turned(bias[:, :key_len], starts[0])
        bias_ref[w, pl.ds(lines, lines)] = turned(bias[:, key_len:], starts[1])

    def as_row(ref):
        return ref[...].reshape(1, atoms)

    def usable_at(mask, position):
        return (
            (mask == 1)
            & (position >= 0)
            & (position < n * atoms)
            & (position < count_ref[0])
        )

    def alive(usable):
        return jnp.broadcast_to(jnp.where(usable, 1.0, 0.0), (8, usable.shape[1]))

    def lanes_from(row, start, size):
        length = row.shape[1]
        return pltpu.roll(row, (length - start) % length, axis=1)[:, :size]

    inner = [
        w
        for w in range(windows)
        if w * query_len >= margin and w * query_len - margin + key_len <= atoms
    ]
    outer = [w for w in range(windows) if w not in inner]
    live = alive(usable_at(as_row(mask_ref), me * atoms + iota((1, atoms), 1)))
    def first_key(w):
        return key_len + w * query_len - margin

    far_keys = (key_len - wide, key_len + atoms + wide - key_len)

    def pairs():
        for w in inner:
            keep = lanes_from(live, w * query_len - margin, key_len)
            pair_window(w, pair_buf[w], [keep, keep], [first_key(w)] * 2)
            yield
        for w in outer:
            pair_window(w, pair_buf[w], None, [first_key(w)] * 2)
            yield

    head_of = iota((half, width), 1) // head_dim
    blank = jnp.zeros((width, key_len), BF16)
    lane = iota((width, key_len), 1)

    def tiles_of(w, s):
        return [(t, first_key(w), w * query_len, query_len, w, 0) for t in (s, s + 1)]

    def far_tiles(s):
        return [
            (s, far_keys[0], atoms, half, windows, 0),
            (s, far_keys[1], atoms + half, half, windows, lines),
        ]

    def stacked(s, row, count):
        query = q_ref[s, pl.ds(row, count)]
        parts = []
        for at in range(0, count, half):
            piece = query[at : at + half]
            for h in range(heads):
                parts.append(jnp.where(head_of == h, piece, jnp.zeros_like(piece)))
        return jnp.concatenate(parts, axis=0)

    def score(tiles):
        both = jnp.concatenate([stacked(s, row, m) for s, _, row, m, _, _ in tiles], axis=1)
        tall = []
        for s, key, _, _, _, _ in tiles:
            line = [blank] * len(tiles)
            t, turn = key // key_len, key % key_len
            line[len(tall)] = jnp.where(lane < turn, keys_ref[s, t + 1], keys_ref[s, t])
            tall.append(jnp.concatenate(line, axis=1))
        scores = mm(both, jnp.concatenate(tall, axis=0))
        found = []
        for i, (_, _, _, m, w, line) in enumerate(tiles):
            own = scores[:, i * key_len : (i + 1) * key_len]
            own = own + bias_ref[w, pl.ds(line, heads * m)]
            found.append((own, jnp.max(own, axis=1, keepdims=True)))
        return found

    def mix(tiles, found):
        mixes = []
        for (s, key, _, _, _, _), (own, top) in zip(tiles, found):
            turn = key % key_len
            split = key + key_len - turn
            value = values_ref[s, pl.ds(key, key_len - turn)]
            if turn:
                value = jnp.concatenate([values_ref[s, pl.ds(split, turn)], value], axis=0)
            mixes.append(mm(jnp.exp(own - top).astype(BF16), value))
        return mixes

    def blend(tiles, mixes):
        for (s, _, row, m, _, _), mixed in zip(tiles, mixes):
            rows = pl.ds(row, m)
            outs = []
            for base in range(0, heads * m, lines):
                value = mixed[base : base + half, :width]
                amount = mixed[base : base + half, width:]
                for h in range(1, heads):
                    at = base + h * half
                    value = jnp.where(head_of == h, mixed[at : at + half, :width], value)
                    amount = jnp.where(head_of == h, mixed[at : at + half, width:], amount)
                outs.append(value / amount)
            blend_ref[s, rows] = (jnp.concatenate(outs, axis=0) * gate_ref[s, rows]).astype(BF16)

    def transition(parts):
        def gather(ref):
            return jnp.concatenate([ref[s, pl.ds(a, m)] for s, a, m in parts], axis=0)

        def modulation(k):
            return jnp.concatenate([mod_ref[k, pl.ds(a, m)] for _, a, m in parts], axis=0)

        mixed = mm(gather(blend_ref), out_ref[...])
        yield
        after = (gather(atoms_ref).astype(F32) + modulation(2) * mixed).astype(BF16)
        trans_in = (norm(after) * modulation(3) + modulation(4)).astype(BF16)
        mixed = mm(trans_in, swiglu_ref[...])
        yield
        units = (jax.nn.silu(mixed[:, :hidden]) * mixed[:, hidden:]).astype(BF16)
        mixed = mm(units, down_ref[...])
        yield
        final = (after.astype(F32) + modulation(5) * mixed).astype(BF16)
        features = jnp.maximum(mm(final, token_weight_ref[...]), 0.0).astype(BF16)
        at = 0
        for s, a, m in parts:
            kept = min(a + m, atoms) - a
            atoms_out_ref[s, pl.ds(a, kept)] = final[at : at + kept]
            feat_ref[s, pl.ds(a, m)] = features[at : at + m]
            at += m
        yield

    def attention(units):
        found, mixes = {}, {}
        for i in range(len(units) + MIX_LAG + BLEND_LAG):
            if i < len(units):
                found[i] = score(units[i])
            j = i - MIX_LAG
            if 0 <= j < len(units):
                mixes[j] = mix(units[j], found.pop(j))
            j = j - BLEND_LAG
            if 0 <= j < len(units):
                blend(units[j], mixes.pop(j))
            yield

    def rotate(streams):
        streams = list(streams)
        while streams:
            for stream in list(streams):
                if next(stream, streams) is streams:
                    streams.remove(stream)
                else:
                    yield

    def series(*streams):
        for stream in streams:
            yield from stream

    def together(main, side, start, every):
        for i, _ in enumerate(main):
            if i >= start and (i - start) % every == 0:
                next(side, None)

    first, count = inner[0] * query_len, len(inner) * query_len
    bias_steps = pairs()
    together(bias_steps, series(projection(2), projection(3)), 1, 2)

    units = [tiles_of(w, s) for s in range(0, samples, 2) for w in inner]
    lag = MIX_LAG + BLEND_LAG
    fill = rotate([transition([(s, first, count)]) for s in range(2)])
    for i, _ in enumerate(attention(units)):
        if i >= len(inner) + lag + T_LATE:
            next(fill, None)
    fill = series(fill, rotate([transition([(s, first, count)]) for s in range(2, samples)]))
    for _ in range(AHEAD):
        next(fill, None)

    for to_there, out_there, in_there in (
        (to_right, has_right, has_left),
        (to_left, has_left, has_right),
    ):

        @pl.when(out_there)
        def _(copies=to_there):
            for copy in copies:
                copy.wait_send()

        @pl.when(in_there)
        def _(copies=to_there):
            for copy in copies:
                copy.wait_recv()

    extent = atoms + 2 * lanes

    def extended(halo, ref):
        return jnp.concatenate(
            [as_row(halo[0])[:, atoms - lanes :], as_row(ref), as_row(halo[1])[:, :lanes]],
            axis=1,
        )

    usable = usable_at(extended(halo_m, mask_ref), me * atoms - lanes + iota((1, extent), 1))
    relative = jnp.where(usable, extended(halo_t, token_ref) - me * tokens, -2)
    live = alive(usable)

    def halo():
        near = [pl.ds(wide - half, half), pl.ds(0, half)]
        for side in range(2):
            atoms_ref[:, pl.ds(atoms + side * half, half)] = halo_x[side, :, near[side]]
        cond_norm = norm(jnp.concatenate([halo_c[0], halo_c[1]], axis=0)).astype(BF16)
        normed = norm(
            jnp.concatenate(
                [halo_x[side].reshape(samples * wide, width) for side in range(2)], axis=0
            )
        ).reshape(2, samples, wide, width)
        adapt = mm(cond_norm, ada_ref[0])
        close = jnp.concatenate([cond_norm[wide - half : wide], cond_norm[wide : wide + half]], axis=0)
        close_adapt = mm(close, ada_ref[1])
        zeroed = mm(close, jnp.concatenate([zero_ref[0], zero_ref[1]], axis=1))
        far = [
            lanes_from(live, lanes - wide, key_len),
            lanes_from(live, lanes + atoms + wide - key_len, key_len),
        ]
        pair_window(windows, pair_far[...], far, far_keys)
        yield
        for w in outer:
            keep = lanes_from(live, lanes + w * query_len - margin, key_len)
            keep = turned(keep, first_key(w))[0:1] > 0.5
            bias_ref[w] = jnp.where(keep, bias_ref[w], DEAD)
        extra = pl.ds(atoms, 2 * half)
        mod_ref[3, extra] = jax.nn.sigmoid(close_adapt[:, :width] + ada_bias_ref[1:2])
        mod_ref[4, extra] = close_adapt[:, width:]
        for which in range(2):
            mod_ref[3 * which + 2, extra] = jax.nn.sigmoid(
                zeroed[:, which * width : (which + 1) * width] + zero_bias_ref[which : which + 1]
            )
        scale = jax.nn.sigmoid(adapt[:, :width] + ada_bias_ref[0:1])
        attn_in = (
            normed * scale.reshape(2, 1, wide, width)
            + adapt[:, width:].reshape(2, 1, wide, width)
        ).astype(BF16)
        projected = mm(
            attn_in.reshape(2 * samples * wide, width), qkvg_ref[:, pl.ds(width, 2 * width)]
        )
        close = jnp.concatenate(
            [
                attn_in[side, s, at : at + half]
                for s in range(samples)
                for side, at in enumerate((wide - half, 0))
            ],
            axis=0,
        )
        sides = mm(
            close,
            jnp.concatenate(
                [qkvg_ref[:, pl.ds(0, width)], qkvg_ref[:, pl.ds(3 * width, width)]], axis=1
            ),
        ).reshape(samples, 2 * half, 2 * width)
        yield
        for side, there in enumerate((has_left, has_right)):
            own = projected[side * samples * wide : (side + 1) * samples * wide]
            own = jnp.where(there, own, 0.0).astype(BF16).reshape(samples, wide, 2 * width)
            start = key_len - wide if side == 0 else key_len + atoms
            values_ref[:, pl.ds(start, wide), pl.ds(0, width)] = own[:, :, width:]
            rest = jnp.zeros((key_len - wide, width), BF16)
            for s in range(samples):
                key = own[s, :, :width]
                key = [rest, key] if side == 0 else [key, rest]
                tile = 0 if side == 0 else atoms // key_len + 1
                keys_ref[s, tile] = jnp.concatenate(key, axis=0).T
        for s in range(samples):
            q_ref[s, extra] = as_query(sides[s, :, :width])
            gate_ref[s, extra] = jax.nn.sigmoid(sides[s, :, width:])
        yield

    strip = iota((1, extent), 1)
    beyond = jnp.where(
        strip < half,
        pltpu.roll(jnp.broadcast_to(relative, (8, extent)), extent - lanes + half, axis=1)[0:1],
        pltpu.roll(jnp.broadcast_to(relative, (8, extent)), extent - lanes - atoms + half, axis=1)[0:1],
    )[:, : 2 * half]
    chosen = jnp.concatenate([relative[:, lanes : lanes + atoms], beyond], axis=1)
    total_atoms = atoms + 2 * half
    hits = iota((tokens, extent), 0) == jnp.broadcast_to(relative, (tokens, extent))
    per_count = 1.0 / jnp.maximum(
        jnp.sum(jnp.where(hits, 1.0, 0.0), axis=1, keepdims=True), 1.0
    )
    onehot = jnp.where(
        iota((tokens, total_atoms), 0) == jnp.broadcast_to(chosen, (tokens, total_atoms)), 1.0, 0.0
    ).astype(BF16)

    def closing(s):
        yield from transition(
            [(s, 0, first), (s, first + count, atoms - first - count + 2 * half)]
        )
        tokens_out_ref[s] = (mm(onehot, feat_ref[s]) * per_count).astype(BF16)
        yield

    for _ in halo():
        for _ in range(FILL_HALO):
            next(fill, None)
    units = []
    for s in range(0, samples, 2):
        units += [tiles_of(w, s) for w in outer] + [far_tiles(s), far_tiles(s + 1)]
    ready = len(units) // 2 + MIX_LAG + BLEND_LAG
    begun = rotate([closing(s) for s in range(samples // 2)])
    for i, _ in enumerate(attention(units)):
        if i >= ready:
            next(begun, None)
        elif i % FILL_EVERY == 0:
            next(fill, None)
    for _ in rotate([begun, fill] + [closing(s) for s in range(samples // 2, samples)]):
        pass


def flush_body(atoms_ref, tokens_ref, atoms_out_ref, tokens_out_ref, sem):
    copies = [
        pltpu.make_async_copy(atoms_ref, atoms_out_ref, sem.at[0]),
        pltpu.make_async_copy(tokens_ref, tokens_out_ref, sem.at[1]),
    ]
    for copy in copies:
        copy.start()
    for copy in copies:
        copy.wait()


def on_device(
    n,
    atoms_in, cond, pair, atom_mask, atom_count, atom_to_token, ada_weight, ada_bias,
    zero_weight, zero_bias, qkvg_weight, query_bias, pair_weight, out_weight,
    swiglu_weight, down_weight, token_weight,
):
    samples, atoms, width = atoms_in.shape
    windows, query_len, channels, key_len = pair.shape
    heads = pair_weight.shape[0]
    wide = (key_len + query_len) // 2
    spread = atoms + query_len
    tokens = atoms // ATOMS_PER_TOKEN
    token_width = token_weight.shape[1]
    half = query_len // 2
    rows_half = half * channels
    vmem = pl.BlockSpec(memory_space=pltpu.VMEM)
    hbm = pl.BlockSpec(memory_space=pltpu.HBM)
    query_bias = query_bias.reshape(1, width)
    staged = (
        cond, ada_weight, ada_bias, zero_weight, zero_bias, qkvg_weight,
        query_bias, pair_weight, out_weight, swiglu_weight, down_weight, token_weight,
        atom_mask, atom_to_token,
    )
    held = pl.pallas_call(
        functools.partial(block_body, n),
        out_shape=(
            pltpu.VMEM(atoms_in.shape, BF16),
            pltpu.VMEM((samples, tokens, token_width), BF16),
        ),
        in_specs=[hbm] * 5 + [pl.BlockSpec(memory_space=pltpu.SMEM)] + [hbm] * 11,
        out_specs=(vmem, vmem),
        scratch_shapes=[pltpu.VMEM(a.shape, a.dtype) for a in staged]
        + [
            pltpu.VMEM((samples, spread, width), BF16),
            pltpu.VMEM((samples, wide, width), BF16),
            pltpu.VMEM((wide, width), BF16),
            pltpu.VMEM((windows, query_len * channels, key_len), BF16),
            pltpu.VMEM((query_len * channels, key_len), BF16),
            pltpu.VMEM((2, samples, wide, width), BF16),
            pltpu.VMEM((2, wide, width), BF16),
            pltpu.VMEM((atoms,), jnp.int32),
            pltpu.VMEM((atoms,), jnp.int32),
            pltpu.VMEM((atoms,), jnp.int32),
            pltpu.VMEM((atoms,), jnp.int32),
            pltpu.VMEM((samples, atoms // key_len + 2, width, key_len), BF16),
            pltpu.VMEM((samples, atoms + 2 * key_len, 2 * width), BF16),
            pltpu.VMEM((samples, spread, width), BF16),
            pltpu.VMEM((samples, spread, width), F32),
            pltpu.VMEM((windows + 1, heads * query_len, key_len), F32),
            pltpu.VMEM((6, spread, width), F32),
            pltpu.VMEM((samples, spread, token_width), BF16),
            pltpu.VMEM((samples, spread, width), BF16),
            pltpu.VMEM((rows_half + 3 * heads * half, rows_half), BF16),
            pltpu.SemaphoreType.DMA((len(staged) + 3,)),
            pltpu.SemaphoreType.DMA((1,)),
            pltpu.SemaphoreType.DMA((2, 5)),
            pltpu.SemaphoreType.DMA((2, 5)),
            pltpu.SemaphoreType.REGULAR,
        ],
        compiler_params=pltpu.CompilerParams(collective_id=0, has_side_effects=True),
        name="atom_block",
    )(
        atoms_in, cond, pair.reshape(windows, query_len * channels, key_len),
        atom_mask, atom_to_token, atom_count,
        ada_weight, ada_bias, zero_weight, zero_bias, qkvg_weight,
        query_bias, pair_weight, out_weight, swiglu_weight,
        down_weight, token_weight,
    )
    return pl.pallas_call(
        flush_body,
        out_shape=tuple(jax.ShapeDtypeStruct(a.shape, a.dtype) for a in held),
        in_specs=[pl.BlockSpec(memory_space=pl.ANY)] * 2,
        out_specs=(hbm, hbm),
        scratch_shapes=[pltpu.SemaphoreType.DMA((2,))],
        name="flush",
    )(*[pltpu.with_memory_space_constraint(a, pltpu.VMEM) for a in held])


def solution(mesh):
    shard = P(("struct", "atom"))
    stream = P("struct", "atom", None)
    in_specs = (stream, shard, shard, shard, P("struct"), shard) + (P(),) * 11
    return jax.shard_map(
        functools.partial(on_device, mesh.shape["atom"]),
        mesh=mesh,
        in_specs=in_specs,
        out_specs=(stream, stream),
        check_vma=False,
    )
```

```python
import functools

import jax
import jax.numpy as jnp
from jax import lax
from jax.experimental import pallas as pl
from jax.experimental.pallas import tpu as pltpu
from jax.sharding import PartitionSpec as P

ATOMS_PER_TOKEN = 8
EPS = 1e-05
DEAD = -1e30
MIX_LAG = 4
BLEND_LAG = 1
AHEAD = 4
T_LATE = 0
PREP_EVERY = 2
MIX_OUT = 4
FILL_HALO = 1
FILL_EVERY = 2
MESH = pl.DeviceIdType.MESH
F32 = jnp.float32
BF16 = jnp.bfloat16


def iota(shape, axis):
    return lax.broadcasted_iota(jnp.int32, shape, axis)


def mm(a, b):
    return jnp.dot(a, b, preferred_element_type=F32)


def block_body(
    n,
    atoms_hbm, cond_hbm, pair_ref, mask_hbm, token_hbm, count_ref,
    ada_hbm, ada_bias_hbm, zero_hbm, zero_bias_hbm, qkvg_hbm, query_bias_hbm,
    pair_weight_hbm, out_hbm, swiglu_hbm, down_hbm, token_weight_hbm,
    atoms_out_ref, tokens_out_ref,
    cond_ref, ada_ref, ada_bias_ref, zero_ref, zero_bias_ref, qkvg_ref,
    query_bias_ref, pair_weight_ref, out_ref, swiglu_ref, down_ref, token_weight_ref,
    mask_ref, token_ref, atoms_ref,
    lead_x, lead_c, pair_buf, pair_far, halo_x, halo_c, halo_m0, halo_m1, halo_t0, halo_t1,
    keys_ref, values_ref, q_ref, gate_ref, bias_ref, mod_ref, feat_ref, blend_ref, lhs_ref,
    load_sem, pair_sem, send_sem, recv_sem, ready_sem,
):
    samples, atoms, width = atoms_out_ref.shape
    windows, rows_pair, key_len = pair_ref.shape
    heads, channels = pair_weight_ref.shape
    head_dim = width // heads
    query_len = rows_pair // channels
    half = query_len // 2
    margin = (key_len - query_len) // 2
    wide = margin + query_len
    reach = ATOMS_PER_TOKEN
    tokens = tokens_out_ref.shape[1]
    hidden = down_ref.shape[0]
    rows_half = half * channels
    lines = heads * half
    lanes = 128

    halo_m, halo_t = (halo_m0, halo_m1), (halo_t0, halo_t1)
    me = lax.axis_index("atom")
    right, left = lax.rem(me + 1, n), lax.rem(me + n - 1, n)

    barrier = pltpu.get_barrier_semaphore()
    has_left, has_right = me > 0, me < n - 1

    @pl.when(has_right)
    def _():
        pl.semaphore_signal(barrier, inc=1, device_id={"atom": right}, device_id_type=MESH)


    pair_copy = pltpu.make_async_copy(pair_ref, pair_buf, pair_sem.at[0])
    early = (
        (atoms_hbm.at[:, pl.ds(0, wide)], lead_x), (cond_hbm.at[pl.ds(0, wide)], lead_c),
        (mask_hbm, mask_ref), (token_hbm, token_ref),
        (atoms_hbm, atoms_ref.at[:, pl.ds(0, atoms)]), (cond_hbm, cond_ref), (ada_hbm, ada_ref),
        (ada_bias_hbm, ada_bias_ref), (zero_hbm, zero_ref), (zero_bias_hbm, zero_bias_ref),
        (qkvg_hbm, qkvg_ref), (query_bias_hbm, query_bias_ref),
        (pair_weight_hbm, pair_weight_ref),
    )
    late = (
        (out_hbm, out_ref), (swiglu_hbm, swiglu_ref), (down_hbm, down_ref),
        (token_weight_hbm, token_weight_ref),
    )
    loads = [
        pltpu.make_async_copy(src, dst, load_sem.at[i])
        for i, (src, dst) in enumerate(early + late)
    ]
    for copy in loads[: len(early)]:
        copy.start()

    inverse = 1.0 / width
    values_ref[:, :, width:] = jnp.ones((samples, atoms + 2 * key_len, width), BF16)
    row, col = iota((rows_half, rows_half), 0), iota((rows_half, rows_half), 1)
    place = (row % half) * channels + row // half
    same = jnp.where(row % half == col // channels, 1.0 / channels, 0.0)
    lhs_ref[pl.ds(0, rows_half)] = (jnp.where(place == col, 1.0, 0.0) - same).astype(BF16)

    skipped = rows_half - reach * channels
    pair_far[pl.ds(0, skipped)] = jnp.zeros((skipped, key_len), BF16)
    pair_far[pl.ds(2 * rows_half - skipped, skipped)] = jnp.zeros((skipped, key_len), BF16)
    for side, there in enumerate((has_left, has_right)):

        @pl.when(jnp.logical_not(there))
        def _(side=side):
            at = skipped + side * reach * channels
            pair_far[pl.ds(at, reach * channels)] = jnp.zeros((reach * channels, key_len), BF16)
            halo_x[side] = jnp.zeros(halo_x.shape[1:], BF16)
            halo_c[side] = jnp.zeros(halo_c.shape[1:], BF16)
            halo_m[side][...] = jnp.zeros(halo_m0.shape, jnp.int32)
            halo_t[side][...] = jnp.zeros(halo_t0.shape, jnp.int32)

    copies = []
    for side, (target, start, far) in enumerate(
        ((right, atoms - wide, (windows - 1, rows_pair - reach * channels)), (left, 0, (0, 0)))
    ):
        own = pl.ds(start, wide)
        size = reach * channels
        for which, (src, dst) in enumerate(
            (
                (lead_x if side else atoms_ref.at[:, own], halo_x.at[side]),
                (lead_c if side else cond_ref.at[own], halo_c.at[side]),
                (mask_ref, halo_m[side]),
                (token_ref, halo_t[side]),
                (
                    pair_ref.at[far[0], pl.ds(far[1], size)],
                    pair_far.at[pl.ds(skipped + side * size, size)],
                ),
            )
        ):
            copies.append(
                pltpu.make_async_remote_copy(
                    src_ref=src,
                    dst_ref=dst,
                    send_sem=send_sem.at[side, which],
                    recv_sem=recv_sem.at[side, which],
                    device_id={"atom": target},
                    device_id_type=MESH,
                )
            )
    to_right, to_left = copies[:5], copies[5:]

    def norm(values):
        values = values.astype(F32)
        centred = values - jnp.sum(values, axis=1, keepdims=True) * inverse
        spread = jnp.sum(centred * centred, axis=1, keepdims=True) * inverse
        return centred * lax.rsqrt(spread + EPS)

    @pl.when(has_left)
    def _():
        pl.semaphore_wait(barrier, 1)
        pl.semaphore_signal(ready_sem, inc=1, device_id={"atom": left}, device_id_type=MESH)

    for copy in loads[:4]:
        copy.wait()

    @pl.when(has_left)
    def _():
        for copy in to_left:
            copy.start()

    pair_copy.start()
    for copy in loads[len(early) :]:
        copy.start()
    for copy in loads[4 : len(early)]:
        copy.wait()

    own = pl.ds(0, atoms)
    factor = head_dim**-0.5

    def as_query(projected):
        return ((projected + query_bias_ref[...]) * factor).astype(BF16)

    def conditioning():
        cond_norm = norm(cond_ref[...]).astype(BF16)
        yield
        for which in range(2):
            adapt = mm(cond_norm, ada_ref[which])
            mod_ref[3 * which, own] = jax.nn.sigmoid(
                adapt[:, :width] + ada_bias_ref[which : which + 1]
            )
            mod_ref[3 * which + 1, own] = adapt[:, width:]
            yield
        zeroed = mm(cond_norm, jnp.concatenate([zero_ref[0], zero_ref[1]], axis=1))
        for which in range(2):
            mod_ref[3 * which + 2, own] = jax.nn.sigmoid(
                zeroed[:, which * width : (which + 1) * width] + zero_bias_ref[which : which + 1]
            )
        yield

    def projection(s):
        normed = norm(atoms_ref[s, own])
        yield
        attn_in = (normed * mod_ref[0, own] + mod_ref[1, own]).astype(BF16)
        projected = mm(attn_in, qkvg_ref[...])
        q_ref[s, own] = as_query(projected[:, :width])
        key = projected[:, width : 2 * width].astype(BF16)
        for t in range(atoms // key_len):
            keys_ref[s, t + 1] = key[t * key_len : (t + 1) * key_len].T
        values_ref[s, pl.ds(key_len, atoms), pl.ds(0, width)] = projected[
            :, 2 * width : 3 * width
        ].astype(BF16)
        gate_ref[s, own] = jax.nn.sigmoid(projected[:, 3 * width :])
        yield

    starts = [conditioning(), projection(0), projection(1)]
    for stream in starts:
        next(stream)

    weight = pair_weight_ref[...]
    weight = weight - jnp.mean(weight, axis=1, keepdims=True)
    spread_c = jnp.where(
        iota((channels, rows_half), 1) % channels == iota((channels, rows_half), 0), 1.0, 0.0
    ).astype(BF16)
    own_query = iota((half, rows_half), 1) // channels == iota((half, rows_half), 0)
    remaining = weight
    for piece in range(3):
        part = remaining.astype(BF16)
        remaining = remaining - part.astype(F32)
        broad = mm(part, spread_c)
        blocks = [
            jnp.where(own_query, jnp.broadcast_to(broad[h : h + 1], (half, rows_half)), 0.0)
            for h in range(heads)
        ]
        lhs_ref[pl.ds(rows_half + piece * lines, lines)] = jnp.concatenate(
            blocks, axis=0
        ).astype(BF16)

    next(starts[0])
    for stream in starts[1:]:
        for _ in stream:
            pass

    @pl.when(has_right)
    def _():
        pl.semaphore_wait(ready_sem, 1)
        for copy in to_right:
            copy.start()

    for copy in loads[len(early) :]:
        copy.wait()
    pair_copy.wait()

    def turned(bias, start):
        turn = start % key_len
        return pltpu.roll(bias, turn, axis=1) if turn else bias

    def pair_window(w, block, keep, starts):
        both = jnp.concatenate([block[:rows_half], block[rows_half:]], axis=1)
        result = mm(lhs_ref[...], both)
        square = None
        for c in range(channels):
            centred = result[c * half : (c + 1) * half]
            square = centred * centred if c == 0 else square + centred * centred
        at = rows_half
        total = (
            result[at : at + lines]
            + result[at + lines : at + 2 * lines]
            + result[at + 2 * lines : at + 3 * lines]
        )
        scale = lax.rsqrt(square * (1.0 / channels) + EPS)
        bias = total * jnp.concatenate([scale] * heads, axis=0)
        if keep is not None:
            bias = jnp.where(jnp.concatenate(keep, axis=1)[0:1] > 0.5, bias, DEAD)
        bias_ref[w, pl.ds(0, lines)] = turned(bias[:, :key_len], starts[0])
        bias_ref[w, pl.ds(lines, lines)] = turned(bias[:, key_len:], starts[1])

    def as_row(ref):
        return ref[...].reshape(1, atoms)

    def usable_at(mask, position):
        return (
            (mask == 1)
            & (position >= 0)
            & (position < n * atoms)
            & (position < count_ref[0])
        )

    def alive(usable):
        return jnp.broadcast_to(jnp.where(usable, 1.0, 0.0), (8, usable.shape[1]))

    def lanes_from(row, start, size):
        length = row.shape[1]
        return pltpu.roll(row, (length - start) % length, axis=1)[:, :size]

    inner = [
        w
        for w in range(windows)
        if w * query_len >= margin and w * query_len - margin + key_len <= atoms
    ]
    outer = [w for w in range(windows) if w not in inner]
    live = alive(usable_at(as_row(mask_ref), me * atoms + iota((1, atoms), 1)))
    def first_key(w):
        return key_len + w * query_len - margin

    far_keys = (key_len - wide, key_len + atoms + wide - key_len)

    def pairs():
        for w in inner:
            keep = lanes_from(live, w * query_len - margin, key_len)
            pair_window(w, pair_buf[w], [keep, keep], [first_key(w)] * 2)
            yield
        for w in outer:
            pair_window(w, pair_buf[w], None, [first_key(w)] * 2)
            yield

    head_of = iota((half, width), 1) // head_dim
    blank = jnp.zeros((width, key_len), BF16)
    lane = iota((width, key_len), 1)

    def tiles_of(w, s):
        return [(t, first_key(w), w * query_len, query_len, w, 0) for t in (s, s + 1)]

    def far_tiles(s):
        return [
            (s, far_keys[0], atoms, half, windows, 0),
            (s, far_keys[1], atoms + half, half, windows, lines),
        ]

    def stacked(s, row, count):
        query = q_ref[s, pl.ds(row, count)]
        parts = []
        for at in range(0, count, half):
            piece = query[at : at + half]
            for h in range(heads):
                parts.append(jnp.where(head_of == h, piece, jnp.zeros_like(piece)))
        return jnp.concatenate(parts, axis=0)

    def score(tiles):
        both = jnp.concatenate([stacked(s, row, m) for s, _, row, m, _, _ in tiles], axis=1)
        tall = []
        for s, key, _, _, _, _ in tiles:
            line = [blank] * len(tiles)
            t, turn = key // key_len, key % key_len
            line[len(tall)] = jnp.where(lane < turn, keys_ref[s, t + 1], keys_ref[s, t])
            tall.append(jnp.concatenate(line, axis=1))
        scores = mm(both, jnp.concatenate(tall, axis=0))
        found = []
        for i, (_, _, _, m, w, line) in enumerate(tiles):
            own = scores[:, i * key_len : (i + 1) * key_len]
            own = own + bias_ref[w, pl.ds(line, heads * m)]
            found.append((own, jnp.max(own, axis=1, keepdims=True)))
        return found

    def mix(tiles, found):
        mixes = []
        for (s, key, _, _, _, _), (own, top) in zip(tiles, found):
            turn = key % key_len
            split = key + key_len - turn
            value = values_ref[s, pl.ds(key, key_len - turn)]
            if turn:
                value = jnp.concatenate([values_ref[s, pl.ds(split, turn)], value], axis=0)
            mixes.append(mm(jnp.exp(own - top).astype(BF16), value))
        return mixes

    def blend(tiles, mixes):
        for (s, _, row, m, _, _), mixed in zip(tiles, mixes):
            rows = pl.ds(row, m)
            outs = []
            for base in range(0, heads * m, lines):
                value = mixed[base : base + half, :width]
                amount = mixed[base : base + half, width:]
                for h in range(1, heads):
                    at = base + h * half
                    value = jnp.where(head_of == h, mixed[at : at + half, :width], value)
                    amount = jnp.where(head_of == h, mixed[at : at + half, width:], amount)
                outs.append(value / amount)
            blend_ref[s, rows] = (jnp.concatenate(outs, axis=0) * gate_ref[s, rows]).astype(BF16)

    def transition(parts):
        def gather(ref):
            return jnp.concatenate([ref[s, pl.ds(a, m)] for s, a, m in parts], axis=0)

        def modulation(k):
            return jnp.concatenate([mod_ref[k, pl.ds(a, m)] for _, a, m in parts], axis=0)

        mixed = mm(gather(blend_ref), out_ref[...])
        yield
        after = (gather(atoms_ref).astype(F32) + modulation(2) * mixed).astype(BF16)
        trans_in = (norm(after) * modulation(3) + modulation(4)).astype(BF16)
        mixed = mm(trans_in, swiglu_ref[...])
        yield
        units = (jax.nn.silu(mixed[:, :hidden]) * mixed[:, hidden:]).astype(BF16)
        mixed = mm(units, down_ref[...])
        yield
        final = (after.astype(F32) + modulation(5) * mixed).astype(BF16)
        features = jnp.maximum(mm(final, token_weight_ref[...]), 0.0).astype(BF16)
        at = 0
        for s, a, m in parts:
            kept = min(a + m, atoms) - a
            atoms_out_ref[s, pl.ds(a, kept)] = final[at : at + kept]
            feat_ref[s, pl.ds(a, m)] = features[at : at + m]
            at += m
        yield

    def attention(units, ahead=MIX_LAG):
        found, mixes = {}, {}
        for i in range(len(units) + ahead + BLEND_LAG):
            if i < len(units):
                found[i] = score(units[i])
            j = i - ahead
            if 0 <= j < len(units):
                mixes[j] = mix(units[j], found.pop(j))
            j = j - BLEND_LAG
            if 0 <= j < len(units):
                blend(units[j], mixes.pop(j))
            yield

    def rotate(streams):
        streams = list(streams)
        while streams:
            for stream in list(streams):
                if next(stream, streams) is streams:
                    streams.remove(stream)
                else:
                    yield

    def series(*streams):
        for stream in streams:
            yield from stream

    def together(main, side, start, every):
        for i, _ in enumerate(main):
            if i >= start and (i - start) % every == 0:
                next(side, None)

    first, count = inner[0] * query_len, len(inner) * query_len
    bias_steps = pairs()
    together(bias_steps, series(projection(2), projection(3), starts[0]), 1, PREP_EVERY)
    for _ in starts[0]:
        pass

    units = [tiles_of(w, s) for s in range(0, samples, 2) for w in inner]
    lag = MIX_LAG + BLEND_LAG
    fill = rotate([transition([(s, first, count)]) for s in range(2)])
    for i, _ in enumerate(attention(units)):
        if i >= len(inner) + lag + T_LATE:
            next(fill, None)
    fill = series(fill, rotate([transition([(s, first, count)]) for s in range(2, samples)]))
    for _ in range(AHEAD):
        next(fill, None)

    for to_there, out_there, in_there in (
        (to_right, has_right, has_left),
        (to_left, has_left, has_right),
    ):

        @pl.when(out_there)
        def _(copies=to_there):
            for copy in copies:
                copy.wait_send()

        @pl.when(in_there)
        def _(copies=to_there):
            for copy in copies:
                copy.wait_recv()

    extent = atoms + 2 * lanes

    def extended(halo, ref):
        return jnp.concatenate(
            [as_row(halo[0])[:, atoms - lanes :], as_row(ref), as_row(halo[1])[:, :lanes]],
            axis=1,
        )

    usable = usable_at(extended(halo_m, mask_ref), me * atoms - lanes + iota((1, extent), 1))
    relative = jnp.where(usable, extended(halo_t, token_ref) - me * tokens, -2)
    live = alive(usable)

    def halo():
        near = [pl.ds(wide - half, half), pl.ds(0, half)]
        for side in range(2):
            atoms_ref[:, pl.ds(atoms + side * half, half)] = halo_x[side, :, near[side]]
        cond_norm = norm(jnp.concatenate([halo_c[0], halo_c[1]], axis=0)).astype(BF16)
        normed = norm(
            jnp.concatenate(
                [halo_x[side].reshape(samples * wide, width) for side in range(2)], axis=0
            )
        ).reshape(2, samples, wide, width)
        adapt = mm(cond_norm, ada_ref[0])
        close = jnp.concatenate([cond_norm[wide - half : wide], cond_norm[wide : wide + half]], axis=0)
        close_adapt = mm(close, ada_ref[1])
        zeroed = mm(close, jnp.concatenate([zero_ref[0], zero_ref[1]], axis=1))
        far = [
            lanes_from(live, lanes - wide, key_len),
            lanes_from(live, lanes + atoms + wide - key_len, key_len),
        ]
        pair_window(windows, pair_far[...], far, far_keys)
        yield
        for w in outer:
            keep = lanes_from(live, lanes + w * query_len - margin, key_len)
            keep = turned(keep, first_key(w))[0:1] > 0.5
            bias_ref[w] = jnp.where(keep, bias_ref[w], DEAD)
        extra = pl.ds(atoms, 2 * half)
        mod_ref[3, extra] = jax.nn.sigmoid(close_adapt[:, :width] + ada_bias_ref[1:2])
        mod_ref[4, extra] = close_adapt[:, width:]
        for which in range(2):
            mod_ref[3 * which + 2, extra] = jax.nn.sigmoid(
                zeroed[:, which * width : (which + 1) * width] + zero_bias_ref[which : which + 1]
            )
        scale = jax.nn.sigmoid(adapt[:, :width] + ada_bias_ref[0:1])
        attn_in = (
            normed * scale.reshape(2, 1, wide, width)
            + adapt[:, width:].reshape(2, 1, wide, width)
        ).astype(BF16)
        projected = mm(
            attn_in.reshape(2 * samples * wide, width), qkvg_ref[:, pl.ds(width, 2 * width)]
        )
        close = jnp.concatenate(
            [
                attn_in[side, s, at : at + half]
                for s in range(samples)
                for side, at in enumerate((wide - half, 0))
            ],
            axis=0,
        )
        sides = mm(
            close,
            jnp.concatenate(
                [qkvg_ref[:, pl.ds(0, width)], qkvg_ref[:, pl.ds(3 * width, width)]], axis=1
            ),
        ).reshape(samples, 2 * half, 2 * width)
        yield
        for side, there in enumerate((has_left, has_right)):
            own = projected[side * samples * wide : (side + 1) * samples * wide]
            own = jnp.where(there, own, 0.0).astype(BF16).reshape(samples, wide, 2 * width)
            start = key_len - wide if side == 0 else key_len + atoms
            values_ref[:, pl.ds(start, wide), pl.ds(0, width)] = own[:, :, width:]
            rest = jnp.zeros((key_len - wide, width), BF16)
            for s in range(samples):
                key = own[s, :, :width]
                key = [rest, key] if side == 0 else [key, rest]
                tile = 0 if side == 0 else atoms // key_len + 1
                keys_ref[s, tile] = jnp.concatenate(key, axis=0).T
        for s in range(samples):
            q_ref[s, extra] = as_query(sides[s, :, :width])
            gate_ref[s, extra] = jax.nn.sigmoid(sides[s, :, width:])
        yield

    strip = iota((1, extent), 1)
    beyond = jnp.where(
        strip < half,
        pltpu.roll(jnp.broadcast_to(relative, (8, extent)), extent - lanes + half, axis=1)[0:1],
        pltpu.roll(jnp.broadcast_to(relative, (8, extent)), extent - lanes - atoms + half, axis=1)[0:1],
    )[:, : 2 * half]
    chosen = jnp.concatenate([relative[:, lanes : lanes + atoms], beyond], axis=1)
    total_atoms = atoms + 2 * half
    hits = iota((tokens, extent), 0) == jnp.broadcast_to(relative, (tokens, extent))
    per_count = 1.0 / jnp.maximum(
        jnp.sum(jnp.where(hits, 1.0, 0.0), axis=1, keepdims=True), 1.0
    )
    onehot = jnp.where(
        iota((tokens, total_atoms), 0) == jnp.broadcast_to(chosen, (tokens, total_atoms)), 1.0, 0.0
    ).astype(BF16)

    def closing(s):
        yield from transition(
            [(s, 0, first), (s, first + count, atoms - first - count + 2 * half)]
        )
        tokens_out_ref[s] = (mm(onehot, feat_ref[s]) * per_count).astype(BF16)
        yield

    for _ in halo():
        for _ in range(FILL_HALO):
            next(fill, None)
    units = []
    for s in range(0, samples, 2):
        units += [far_tiles(s), far_tiles(s + 1)] + [tiles_of(w, s) for w in outer]
    ready = len(units) // 2 + MIX_OUT + BLEND_LAG
    begun = rotate([closing(s) for s in range(samples // 2)])
    for i, _ in enumerate(attention(units, MIX_OUT)):
        if i >= ready:
            next(begun, None)
        elif i % FILL_EVERY == 0:
            next(fill, None)
    for _ in rotate([begun, fill] + [closing(s) for s in range(samples // 2, samples)]):
        pass


def flush_body(atoms_ref, tokens_ref, atoms_out_ref, tokens_out_ref, sem):
    copies = [
        pltpu.make_async_copy(atoms_ref, atoms_out_ref, sem.at[0]),
        pltpu.make_async_copy(tokens_ref, tokens_out_ref, sem.at[1]),
    ]
    for copy in copies:
        copy.start()
    for copy in copies:
        copy.wait()


def on_device(
    n,
    atoms_in, cond, pair, atom_mask, atom_count, atom_to_token, ada_weight, ada_bias,
    zero_weight, zero_bias, qkvg_weight, query_bias, pair_weight, out_weight,
    swiglu_weight, down_weight, token_weight,
):
    samples, atoms, width = atoms_in.shape
    windows, query_len, channels, key_len = pair.shape
    heads = pair_weight.shape[0]
    wide = (key_len + query_len) // 2
    spread = atoms + query_len
    tokens = atoms // ATOMS_PER_TOKEN
    token_width = token_weight.shape[1]
    half = query_len // 2
    rows_half = half * channels
    vmem = pl.BlockSpec(memory_space=pltpu.VMEM)
    hbm = pl.BlockSpec(memory_space=pltpu.HBM)
    query_bias = query_bias.reshape(1, width)
    staged = (
        cond, ada_weight, ada_bias, zero_weight, zero_bias, qkvg_weight,
        query_bias, pair_weight, out_weight, swiglu_weight, down_weight, token_weight,
        atom_mask, atom_to_token,
    )
    held = pl.pallas_call(
        functools.partial(block_body, n),
        out_shape=(
            pltpu.VMEM(atoms_in.shape, BF16),
            pltpu.VMEM((samples, tokens, token_width), BF16),
        ),
        in_specs=[hbm] * 5 + [pl.BlockSpec(memory_space=pltpu.SMEM)] + [hbm] * 11,
        out_specs=(vmem, vmem),
        scratch_shapes=[pltpu.VMEM(a.shape, a.dtype) for a in staged]
        + [
            pltpu.VMEM((samples, spread, width), BF16),
            pltpu.VMEM((samples, wide, width), BF16),
            pltpu.VMEM((wide, width), BF16),
            pltpu.VMEM((windows, query_len * channels, key_len), BF16),
            pltpu.VMEM((query_len * channels, key_len), BF16),
            pltpu.VMEM((2, samples, wide, width), BF16),
            pltpu.VMEM((2, wide, width), BF16),
            pltpu.VMEM((atoms,), jnp.int32),
            pltpu.VMEM((atoms,), jnp.int32),
            pltpu.VMEM((atoms,), jnp.int32),
            pltpu.VMEM((atoms,), jnp.int32),
            pltpu.VMEM((samples, atoms // key_len + 2, width, key_len), BF16),
            pltpu.VMEM((samples, atoms + 2 * key_len, 2 * width), BF16),
            pltpu.VMEM((samples, spread, width), BF16),
            pltpu.VMEM((samples, spread, width), F32),
            pltpu.VMEM((windows + 1, heads * query_len, key_len), F32),
            pltpu.VMEM((6, spread, width), F32),
            pltpu.VMEM((samples, spread, token_width), BF16),
            pltpu.VMEM((samples, spread, width), BF16),
            pltpu.VMEM((rows_half + 3 * heads * half, rows_half), BF16),
            pltpu.SemaphoreType.DMA((len(staged) + 3,)),
            pltpu.SemaphoreType.DMA((1,)),
            pltpu.SemaphoreType.DMA((2, 5)),
            pltpu.SemaphoreType.DMA((2, 5)),
            pltpu.SemaphoreType.REGULAR,
        ],
        compiler_params=pltpu.CompilerParams(collective_id=0, has_side_effects=True),
        name="atom_block",
    )(
        atoms_in, cond, pair.reshape(windows, query_len * channels, key_len),
        atom_mask, atom_to_token, atom_count,
        ada_weight, ada_bias, zero_weight, zero_bias, qkvg_weight,
        query_bias, pair_weight, out_weight, swiglu_weight,
        down_weight, token_weight,
    )
    return pl.pallas_call(
        flush_body,
        out_shape=tuple(jax.ShapeDtypeStruct(a.shape, a.dtype) for a in held),
        in_specs=[pl.BlockSpec(memory_space=pl.ANY)] * 2,
        out_specs=(hbm, hbm),
        scratch_shapes=[pltpu.SemaphoreType.DMA((2,))],
        name="flush",
    )(*[pltpu.with_memory_space_constraint(a, pltpu.VMEM) for a in held])


def solution(mesh):
    shard = P(("struct", "atom"))
    stream = P("struct", "atom", None)
    in_specs = (stream, shard, shard, shard, P("struct"), shard) + (P(),) * 11
    return jax.shard_map(
        functools.partial(on_device, mesh.shape["atom"]),
        mesh=mesh,
        in_specs=in_specs,
        out_specs=(stream, stream),
        check_vma=False,
    )
```
